16 devices in a mesh: req: 2 (over y, z), cp: 8 (over x, core).
Axes of the slice: x: 4, y: 2, z: 1, core: 2. Of those that a mesh axis runs over, the one named last changes fastest.
The devices are a block of a 4x4x8 slice.
Arguments:
- hidden: bfloat16 [8192, 2048], P(('req', 'cp')), parts along dimension 0
- positions: int32 [8192], P(('req', 'cp')), parts along dimension 0
- gain_attn: bfloat16 [2, 2048], replicated
- gain_mlp: bfloat16 [2, 2048], replicated
- w_query: bfloat16 [2, 2048, 16, 128], replicated
- w_key: bfloat16 [2, 2048, 16, 128], replicated
- w_value: bfloat16 [2, 2048, 16, 128], replicated
- w_out: bfloat16 [2, 16, 128, 2048], replicated
- w_gate: bfloat16 [2, 2048, 8192], replicated
- w_up: bfloat16 [2, 2048, 8192], replicated
- w_down: bfloat16 [2, 8192, 2048], replicated
Outputs:
- output 1: bfloat16 [8192, 2048], P(('req', 'cp')), parts along dimension 0
- output 2: bfloat16 [2, 8192, 16, 128], P(None, 'req', 'cp'), parts along dimension 1
- output 3: bfloat16 [2, 8192, 16, 128], P(None, 'req', 'cp'), parts along dimension 1
There are 2 independent parts. The reference program is written for one: setup_inputs(seed, part) draws one part's arguments, and reference() takes and returns one part's arrays. A program takes and returns all parts, laid end to end along the dimension named above; an argument that names none is the same for every part.
All inputs are finite; a program needn't handle non-finite values.
Results may differ from the reference program's by a relative error of at most 0.016795.
Values are sent between devices in bfloat16 or wider.
A program may use at most 768 MiB of HBM per device.

```python
import jax
import jax.numpy as jnp
from jax import lax

MODEL_DIM = 2048
NUM_HEADS = 16
KV_HEADS = 16
HEAD_DIM = 128
FFN_DIM = 8192
NUM_LAYERS = 2
TOKENS_DEV = 512
CP_SIZE = 8

SEQ_LEN = CP_SIZE * TOKENS_DEV
CHUNK_LEN = TOKENS_DEV // 2
GROUP_SIZE = NUM_HEADS // KV_HEADS
NORM_EPS = 1e-5
ROPE_BASE = 10000.0


def draw_positions(pos_key):
    step_sizes = jax.random.randint(pos_key, (SEQ_LEN,), 1, 4, dtype=jnp.int32)
    natural = (jnp.cumsum(step_sizes) - step_sizes[0]).astype(jnp.int32)
    halves = natural.reshape(2, CP_SIZE, CHUNK_LEN)
    return jnp.stack([halves[0], halves[1][::-1]], axis=1).reshape(SEQ_LEN)


def setup_inputs(seed: int = 0, part: int = 0) -> dict:
    base_key = jax.random.key(seed)
    part_key = jax.random.fold_in(base_key, part)
    hidden_key, pos_key = jax.random.split(part_key, 2)
    weight_keys = jax.random.split(base_key, 9)
    dim_scale = MODEL_DIM ** -0.5
    shape_q = (NUM_LAYERS, MODEL_DIM, NUM_HEADS, HEAD_DIM)
    shape_kv = (NUM_LAYERS, MODEL_DIM, KV_HEADS, HEAD_DIM)
    shape_ff = (NUM_LAYERS, MODEL_DIM, FFN_DIM)
    shape_gain = (NUM_LAYERS, MODEL_DIM)
    hidden = jax.random.normal(hidden_key, (SEQ_LEN, MODEL_DIM), jnp.float32)
    gain_attn = 1.0 + 0.3 * jax.random.normal(weight_keys[0], shape_gain, jnp.float32)
    gain_mlp = 1.0 + 0.3 * jax.random.normal(weight_keys[1], shape_gain, jnp.float32)
    w_query = 1.5 * dim_scale * jax.random.normal(weight_keys[2], shape_q, jnp.float32)
    w_key = 1.5 * dim_scale * jax.random.normal(weight_keys[3], shape_kv, jnp.float32)
    w_value = dim_scale * jax.random.normal(weight_keys[4], shape_kv, jnp.float32)
    w_out = (NUM_HEADS * HEAD_DIM) ** -0.5 * jax.random.normal(weight_keys[5], (NUM_LAYERS, NUM_HEADS, HEAD_DIM, MODEL_DIM), jnp.float32)
    w_gate = dim_scale * jax.random.normal(weight_keys[6], shape_ff, jnp.float32)
    w_up = dim_scale * jax.random.normal(weight_keys[7], shape_ff, jnp.float32)
    w_down = FFN_DIM ** -0.5 * jax.random.normal(weight_keys[8], (NUM_LAYERS, FFN_DIM, MODEL_DIM), jnp.float32)
    return {
        "hidden": hidden.astype(jnp.bfloat16),
        "positions": draw_positions(pos_key),
        "gain_attn": gain_attn.astype(jnp.bfloat16),
        "gain_mlp": gain_mlp.astype(jnp.bfloat16),
        "w_query": w_query.astype(jnp.bfloat16),
        "w_key": w_key.astype(jnp.bfloat16),
        "w_value": w_value.astype(jnp.bfloat16),
        "w_out": w_out.astype(jnp.bfloat16),
        "w_gate": w_gate.astype(jnp.bfloat16),
        "w_up": w_up.astype(jnp.bfloat16),
        "w_down": w_down.astype(jnp.bfloat16),
    }


def rms_norm(values, gain_vec):
    wide_vals = values.astype(jnp.float32)
    inv_rms = lax.rsqrt(jnp.mean(wide_vals * wide_vals, axis=-1, keepdims=True) + NORM_EPS)
    return (wide_vals * inv_rms * gain_vec.astype(jnp.float32)).astype(jnp.bfloat16)


def rope_tables(pos_vec, head_dim):
    inv_freq = ROPE_BASE ** (-jnp.arange(0, head_dim, 2, dtype=jnp.float32) / head_dim)
    angles = pos_vec.astype(jnp.float32)[..., None] * inv_freq
    return jnp.cos(angles)[..., None, :], jnp.sin(angles)[..., None, :]


def rotate_half(values, cos_tab, sin_tab):
    half_dim = values.shape[-1] // 2
    lower_half = values[..., :half_dim]
    upper_half = values[..., half_dim:]
    return jnp.concatenate([lower_half * cos_tab - upper_half * sin_tab, upper_half * cos_tab + lower_half * sin_tab], axis=-1)


def to_natural(rows):
    split_rows = rows.reshape((CP_SIZE, 2, CHUNK_LEN) + rows.shape[1:])
    return jnp.concatenate([split_rows[:, 0], split_rows[::-1, 1]], axis=0).reshape(rows.shape)


def decoder_layer(hidden, layer_weights, cos_tab, sin_tab, positions):
    gain_attn, gain_mlp, w_query, w_key, w_value, w_out, w_gate, w_up, w_down = layer_weights
    normed = rms_norm(hidden, gain_attn)
    q_proj = jnp.dot(normed, w_query.reshape(MODEL_DIM, NUM_HEADS * HEAD_DIM), preferred_element_type=jnp.float32)
    queries = rotate_half(q_proj.reshape(SEQ_LEN, NUM_HEADS, HEAD_DIM), cos_tab, sin_tab).astype(jnp.bfloat16)
    k_proj = jnp.dot(normed, w_key.reshape(MODEL_DIM, KV_HEADS * HEAD_DIM), preferred_element_type=jnp.float32)
    key_rot = rotate_half(k_proj.reshape(SEQ_LEN, KV_HEADS, HEAD_DIM), cos_tab, sin_tab).astype(jnp.bfloat16)
    v_proj = jnp.dot(normed, w_value.reshape(MODEL_DIM, KV_HEADS * HEAD_DIM), preferred_element_type=jnp.float32)
    value_proj = v_proj.astype(jnp.bfloat16).reshape(SEQ_LEN, KV_HEADS, HEAD_DIM)
    key_wide = key_rot.astype(jnp.float32)
    value_wide = value_proj.astype(jnp.float32)
    q_blocks = queries.reshape(CP_SIZE, TOKENS_DEV, KV_HEADS, GROUP_SIZE, HEAD_DIM)
    pos_blocks = positions.reshape(CP_SIZE, TOKENS_DEV)

    def attend_block(block_in):
        q_block, pos_block = block_in
        scores = jnp.einsum("tkgd,skd->kgts", q_block.astype(jnp.float32), key_wide) * (HEAD_DIM ** -0.5)
        allowed = positions[None, :] <= pos_block[:, None]
        scores = jnp.where(allowed, scores, -jnp.inf)
        row_max = jnp.max(scores, axis=-1, keepdims=True)
        exp_scores = jnp.exp(scores - row_max)
        attn_probs = (exp_scores / jnp.sum(exp_scores, axis=-1, keepdims=True)).astype(jnp.bfloat16)
        return jnp.einsum("kgts,skd->tkgd", attn_probs.astype(jnp.float32), value_wide).astype(jnp.bfloat16)

    attn_out = lax.map(attend_block, (q_blocks, pos_blocks)).reshape(SEQ_LEN, NUM_HEADS * HEAD_DIM)
    attn_proj = jnp.dot(attn_out, w_out.reshape(NUM_HEADS * HEAD_DIM, MODEL_DIM), preferred_element_type=jnp.float32)
    hidden = (hidden.astype(jnp.float32) + attn_proj).astype(jnp.bfloat16)
    normed_mlp = rms_norm(hidden, gain_mlp)
    gate_act = jnp.dot(normed_mlp, w_gate, preferred_element_type=jnp.float32)
    up_act = jnp.dot(normed_mlp, w_up, preferred_element_type=jnp.float32)
    mlp_hidden = (jax.nn.silu(gate_act) * up_act).astype(jnp.bfloat16)
    mlp_out = jnp.dot(mlp_hidden, w_down, preferred_element_type=jnp.float32)
    hidden = (hidden.astype(jnp.float32) + mlp_out).astype(jnp.bfloat16)
    return hidden, key_rot, value_proj


def reference(hidden, positions, gain_attn, gain_mlp, w_query, w_key, w_value, w_out, w_gate, w_up, w_down):
    cos_tab, sin_tab = rope_tables(positions, HEAD_DIM)

    def layer_step(carry_hidden, layer_weights):
        new_hidden, key_rot, value_proj = decoder_layer(carry_hidden, layer_weights, cos_tab, sin_tab, positions)
        return new_hidden, (to_natural(key_rot), to_natural(value_proj))

    stacked = (gain_attn, gain_mlp, w_query, w_key, w_value, w_out, w_gate, w_up, w_down)
    final_hidden, caches = lax.scan(layer_step, hidden, stacked)
    k_cache, v_cache = caches
    return final_hidden, k_cache, v_cache
```

```python
import functools

import jax
import jax.numpy as jnp
from jax import lax
from jax.experimental import pallas as pl
from jax.experimental.pallas import tpu as pltpu
from jax.sharding import PartitionSpec as P

NORM_EPS = 1e-5
ROPE_BASE = 10000.0
LOG2E = 1.4426950408889634
TK = 512


def rms_norm(values, gain_vec):
    wide_vals = values.astype(jnp.float32)
    inv_rms = lax.rsqrt(jnp.mean(wide_vals * wide_vals, axis=-1, keepdims=True) + NORM_EPS)
    return (wide_vals * inv_rms * gain_vec.astype(jnp.float32)).astype(jnp.bfloat16)


def rope_tables(pos_vec, head_dim):
    inv_freq = ROPE_BASE ** (-jnp.arange(0, head_dim, 2, dtype=jnp.float32) / head_dim)
    angles = pos_vec.astype(jnp.float32)[..., None] * inv_freq
    cos, sin = jnp.cos(angles), jnp.sin(angles)
    return jnp.concatenate([cos, cos], axis=-1), jnp.concatenate([-sin, sin], axis=-1)


def qkv_kernel(heads, dim, aliased, h_ref, w_ref, cos_ref, sin_ref, *refs):
    q_ref, k_ref, vt_ref, kc_ref, vc_ref = refs[2:] if aliased else refs
    y = jnp.dot(h_ref[...], w_ref[...], preferred_element_type=jnp.float32)
    cos, sin = cos_ref[...], sin_ref[...]
    width = heads * dim

    def rope(x):
        return x * cos + pltpu.roll(x, dim // 2, 1) * sin

    keys = []
    for n in range(heads):
        lo, hi = n * dim, (n + 1) * dim
        q_ref[:, lo:hi] = rope(y[:, lo:hi]).astype(jnp.bfloat16)
        keys.append(rope(y[:, width + lo : width + hi]))
        k_ref[:, lo:hi] = keys[n].astype(jnp.bfloat16)
    vals = y[:, 2 * width :]
    vt_ref[...] = vals.T.astype(jnp.bfloat16)
    kc_ref[0] = jnp.stack(keys, axis=1).astype(jnp.bfloat16)
    vc_ref[0] = jnp.stack([vals[:, n * dim : (n + 1) * dim] for n in range(heads)], axis=1).astype(jnp.bfloat16)


def qkv(hidden_all, weights, cos, sin, caches, cache_shape, layer, first, reverse, block):
    rows, model = hidden_all.shape
    heads, dim = cache_shape[2], cache_shape[3]
    width = heads * dim
    n = rows // block
    place = (lambda i: n - 1 - i) if reverse else (lambda i: i)
    cache = jax.ShapeDtypeStruct(cache_shape, jnp.bfloat16)
    cache_spec = pl.BlockSpec((1, block, heads, dim), lambda i: (layer, first + place(i), 0, 0))
    args = [hidden_all, weights, cos, sin]
    in_specs = [
        pl.BlockSpec((block, model), lambda i: (i, 0)),
        pl.BlockSpec((model, 3 * width), lambda i: (0, 0)),
        pl.BlockSpec((block, dim), lambda i: (first + place(i), 0)),
        pl.BlockSpec((block, dim), lambda i: (first + place(i), 0)),
    ]
    alias = {}
    if caches is not None:
        args += list(caches)
        in_specs += [pl.BlockSpec(memory_space=pl.ANY)] * 2
        alias = {4: 3, 5: 4}
    return pl.pallas_call(
        functools.partial(qkv_kernel, heads, dim, caches is not None),
        grid=(n,),
        out_shape=[
            jax.ShapeDtypeStruct((rows, width), jnp.bfloat16),
            jax.ShapeDtypeStruct((rows, width), jnp.bfloat16),
            jax.ShapeDtypeStruct((width, rows), jnp.bfloat16),
            cache,
            cache,
        ],
        in_specs=in_specs,
        out_specs=[
            pl.BlockSpec((block, width), lambda i: (place(i), 0)),
            pl.BlockSpec((block, width), lambda i: (place(i), 0)),
            pl.BlockSpec((width, block), lambda i: (0, place(i))),
            cache_spec,
            cache_spec,
        ],
        input_output_aliases=alias,
        compiler_params=pltpu.CompilerParams(vmem_limit_bytes=40 * 1024 * 1024),
        cost_estimate=pl.CostEstimate(flops=2 * rows * model * 3 * width, bytes_accessed=rows * model * 2, transcendentals=0),
    )(*args)


def attn_kernel(heads, dim, parts, q_ref, *refs):
    o_ref = refs[-1]
    kv = [(refs[2 * p], refs[2 * p + 1]) for p in range(parts)]
    tq = q_ref.shape[0]
    qb = pl.program_id(0)
    scale = LOG2E * dim**-0.5
    queries = [q_ref[:, n * dim : (n + 1) * dim] for n in range(heads)]

    def chunk(k_ref, vt_ref, start, carry, masked):
        out = []
        for n in range(heads):
            m, l, acc = carry[n]
            k = k_ref[pl.ds(start, TK), n * dim : (n + 1) * dim]
            s = lax.dot_general(k, queries[n], (((1,), (1,)), ((), ())), preferred_element_type=jnp.float32)
            if masked:
                row = start + lax.broadcasted_iota(jnp.int32, s.shape, 0)
                col = qb * tq + lax.broadcasted_iota(jnp.int32, s.shape, 1)
                s = jnp.where(row <= col, s, -jnp.inf)
            m_new = jnp.maximum(m, jnp.max(s, axis=0, keepdims=True))
            a = jnp.exp2((m - m_new) * scale)
            p = jnp.exp2((s - m_new) * scale)
            l = l * a + jnp.sum(p, axis=0, keepdims=True)
            vt = vt_ref[n * dim : (n + 1) * dim, pl.ds(start, TK)]
            acc = acc * a + jnp.dot(vt, p.astype(jnp.bfloat16), preferred_element_type=jnp.float32)
            out.append((m_new, l, acc))
        return tuple(out)

    carry = tuple(
        (jnp.full((1, tq), -jnp.inf, jnp.float32), jnp.zeros((1, tq), jnp.float32), jnp.zeros((dim, tq), jnp.float32))
        for _ in range(heads)
    )
    if parts == 2:
        k_ref, vt_ref = kv[0]
        carry = lax.fori_loop(
            0, k_ref.shape[0] // TK, lambda j, c: chunk(k_ref, vt_ref, pl.multiple_of(j * TK, TK), c, False), carry
        )
    k_last, vt_last = kv[-1]
    full = (qb * tq) // TK
    carry = lax.fori_loop(0, full, lambda j, c: chunk(k_last, vt_last, pl.multiple_of(j * TK, TK), c, False), carry)
    carry = chunk(k_last, vt_last, pl.multiple_of(full * TK, TK), carry, True)
    for n in range(heads):
        m, l, acc = carry[n]
        o_ref[:, n * dim : (n + 1) * dim] = (acc / l).T.astype(jnp.bfloat16)


def attention(q, kv, heads, dim, block, reverse):
    rows, width = q.shape
    n = rows // block
    place = (lambda i: n - 1 - i) if reverse else (lambda i: i)
    args = [q]
    in_specs = [pl.BlockSpec((block, width), lambda i: (i, 0))]
    for k, vt in kv:
        args += [k, vt]
        in_specs += [pl.BlockSpec(k.shape, lambda i: (0, 0)), pl.BlockSpec(vt.shape, lambda i: (0, 0))]
    pairs = rows * rows * (2 * len(kv) - 1) // 2
    return pl.pallas_call(
        functools.partial(attn_kernel, heads, dim, len(kv)),
        grid=(n,),
        out_shape=jax.ShapeDtypeStruct((rows, width), jnp.bfloat16),
        in_specs=in_specs,
        out_specs=pl.BlockSpec((block, width), lambda i: (place(i), 0)),
        compiler_params=pltpu.CompilerParams(vmem_limit_bytes=40 * 1024 * 1024),
        cost_estimate=pl.CostEstimate(flops=4 * pairs * width, bytes_accessed=rows * width * 8, transcendentals=pairs * heads),
    )(*args)


def solution(mesh):
    cp_size = mesh.shape["cp"]
    row_spec = P(("req", "cp"), None)
    pos_spec = P(("req", "cp"))
    rep_spec = P()
    cache_spec = P(None, "req", "cp", None)

    def per_device(hidden, positions, gain_attn, gain_mlp, w_query, w_key, w_value, w_out, w_gate, w_up, w_down):
        num_layers, model, all_heads, dim = w_query.shape
        heads = all_heads // cp_size
        width = heads * dim
        rows = hidden.shape[0]
        block = rows // 2
        half = cp_size * block
        cache_shape = (num_layers, 2 * half, heads, dim)
        me = lax.axis_index("cp")

        def mine(w):
            return lax.dynamic_slice_in_dim(w, me * heads, heads, 2).reshape(num_layers, model, width)

        w_all = jnp.concatenate([mine(w_query), mine(w_key), mine(w_value)], axis=2)
        pos_all = lax.all_gather(positions, "cp", tiled=False)
        hidden, pos_all = lax.optimization_barrier((hidden, pos_all))
        pos_nat = jnp.concatenate([pos_all[:, :block].reshape(-1), pos_all[::-1, block:].reshape(-1)])
        cos, sin = rope_tables(pos_nat, dim)
        caches = None
        for layer in range(num_layers):
            normed = rms_norm(hidden, gain_attn[layer])
            h_a = lax.all_gather(normed[:block], "cp", tiled=True)
            h_b = lax.all_gather(normed[block:], "cp", tiled=True)
            q_a, k_a, vt_a, *caches = qkv(h_a, w_all[layer], cos, sin, caches, cache_shape, layer, 0, False, block)
            o_a = attention(q_a, [(k_a, vt_a)], heads, dim, block, False)
            o_a = lax.all_to_all(o_a, "cp", 0, 1, tiled=True)
            q_b, k_b, vt_b, *caches = qkv(h_b, w_all[layer], cos, sin, caches, cache_shape, layer, cp_size, True, block)
            o_b = attention(q_b, [(k_a, vt_a), (k_b, vt_b)], heads, dim, block, True)
            o_b = lax.all_to_all(o_b, "cp", 0, 1, tiled=True)
            attn_out = jnp.concatenate([o_a, o_b], axis=0)
            attn_proj = jnp.dot(attn_out, w_out[layer].reshape(all_heads * dim, model), preferred_element_type=jnp.float32)
            hidden = (hidden.astype(jnp.float32) + attn_proj).astype(jnp.bfloat16)
            normed_mlp = rms_norm(hidden, gain_mlp[layer])
            gate_act = jnp.dot(normed_mlp, w_gate[layer], preferred_element_type=jnp.float32)
            up_act = jnp.dot(normed_mlp, w_up[layer], preferred_element_type=jnp.float32)
            mlp_hidden = (jax.nn.silu(gate_act) * up_act).astype(jnp.bfloat16)
            mlp_out = jnp.dot(mlp_hidden, w_down[layer], preferred_element_type=jnp.float32)
            hidden = (hidden.astype(jnp.float32) + mlp_out).astype(jnp.bfloat16)
        return hidden, caches[0], caches[1]

    in_specs = (row_spec, pos_spec) + (rep_spec,) * 9
    return jax.shard_map(per_device, mesh=mesh, in_specs=in_specs, out_specs=(row_spec, cache_spec, cache_spec), check_vma=False)
```

```python
import functools

import jax
import jax.numpy as jnp
from jax import lax
from jax.experimental import pallas as pl
from jax.experimental.pallas import tpu as pltpu
from jax.sharding import PartitionSpec as P

NORM_EPS = 1e-5
ROPE_BASE = 10000.0
LOG2E = 1.4426950408889634
MESH = pl.DeviceIdType.MESH
MIB = 1024 * 1024
TQ = 512
TK = 1024
TF = 1024
BF16, F32 = jnp.bfloat16, jnp.float32


def rms_norm(values, gain_vec):
    wide_vals = values.astype(F32)
    inv_rms = lax.rsqrt(jnp.mean(wide_vals * wide_vals, axis=-1, keepdims=True) + NORM_EPS)
    return (wide_vals * inv_rms * gain_vec.astype(F32)).astype(BF16)


def rope_tables(pos_vec, head_dim):
    inv_freq = ROPE_BASE ** (-jnp.arange(0, head_dim, 2, dtype=F32) / head_dim)
    angles = pos_vec.astype(F32)[..., None] * inv_freq
    cos, sin = jnp.cos(angles), jnp.sin(angles)
    return jnp.concatenate([cos, cos], axis=-1), jnp.concatenate([-sin, sin], axis=-1)


def greet_all(n, me):
    barrier = pltpu.get_barrier_semaphore()
    for d in range(1, n):
        pl.semaphore_signal(barrier, inc=1, device_id={"cp": lax.rem(me + d, n)}, device_id_type=MESH)
    pl.semaphore_wait(barrier, n - 1)


def share_kernel(n, x_ref, o_ref, local_sem, send_sem, recv_sem):
    me = lax.axis_index("cp")
    greet_all(n, me)
    own = pltpu.make_async_copy(x_ref, o_ref.at[me], local_sem)
    own.start()

    def copy(d, slot):
        return pltpu.make_async_remote_copy(
            src_ref=x_ref, dst_ref=o_ref.at[slot], send_sem=send_sem.at[d], recv_sem=recv_sem.at[slot],
            device_id={"cp": lax.rem(me + d, n)}, device_id_type=MESH,
        )

    for d in range(1, n):
        copy(d, me).start()
    own.wait()
    for d in range(1, n):
        copy(d, me).wait_send()
        copy(d, lax.rem(me + d, n)).wait_recv()


def share(x, n):
    return pl.pallas_call(
        functools.partial(share_kernel, n),
        name="share",
        out_shape=jax.ShapeDtypeStruct((n,) + x.shape, x.dtype),
        in_specs=[pl.BlockSpec(memory_space=pltpu.VMEM)],
        out_specs=pl.BlockSpec(memory_space=pltpu.VMEM),
        scratch_shapes=[pltpu.SemaphoreType.DMA, pltpu.SemaphoreType.DMA((n,)), pltpu.SemaphoreType.DMA((n,))],
        compiler_params=pltpu.CompilerParams(collective_id=0, has_side_effects=True),
    )(x)


def qkv_kernel(heads, dim, aliased, ha_ref, hb_ref, w_ref, cos_ref, sin_ref, *refs):
    q_ref, k_ref, vt_ref, kc_ref, vc_ref = refs[2:] if aliased else refs
    h = jnp.concatenate([ha_ref[...], hb_ref[...]], axis=0)
    cos, sin = cos_ref[...], sin_ref[...]
    width = heads * dim

    def project(part):
        return jnp.dot(h, w_ref[:, part * width : (part + 1) * width], preferred_element_type=F32)

    def rope(x):
        return x * cos + pltpu.roll(x, dim // 2, 1) * sin

    y = project(1)
    keys = [rope(y[:, n * dim : (n + 1) * dim]) for n in range(heads)]
    for n in range(heads):
        k_ref[:, n * dim : (n + 1) * dim] = keys[n].astype(BF16)
    kc_ref[0] = jnp.stack(keys, axis=1).astype(BF16)
    y = project(2)
    vt_ref[...] = y.T.astype(BF16)
    vc_ref[0] = jnp.stack([y[:, n * dim : (n + 1) * dim] for n in range(heads)], axis=1).astype(BF16)
    y = project(0)
    for n in range(heads):
        q_ref[:, n * dim : (n + 1) * dim] = rope(y[:, n * dim : (n + 1) * dim]).astype(BF16)


def qkv(hidden_all, weights, cos, sin, caches, cache_shape, layer, first, reverse, block):
    rows, model = hidden_all.shape
    heads, dim = cache_shape[2], cache_shape[3]
    width = heads * dim
    n = rows // block
    tile = 2 * block
    place = (lambda b: n - 1 - b) if reverse else (lambda b: b)
    first = first // 2
    cache = jax.ShapeDtypeStruct(cache_shape, BF16)
    cache_spec = pl.BlockSpec((1, tile, heads, dim), lambda i: (layer, first + i, 0, 0))
    args = [hidden_all, hidden_all, weights, cos, sin]
    in_specs = [
        pl.BlockSpec((block, model), lambda i: (place(2 * i), 0)),
        pl.BlockSpec((block, model), lambda i: (place(2 * i + 1), 0)),
        pl.BlockSpec((model, 3 * width), lambda i: (0, 0)),
        pl.BlockSpec((tile, dim), lambda i: (first + i, 0)),
        pl.BlockSpec((tile, dim), lambda i: (first + i, 0)),
    ]
    alias = {}
    if caches is not None:
        args += list(caches)
        in_specs += [pl.BlockSpec(memory_space=pl.ANY)] * 2
        alias = {5: 3, 6: 4}
    return pl.pallas_call(
        functools.partial(qkv_kernel, heads, dim, caches is not None),
        name="qkv",
        grid=(n // 2,),
        out_shape=[
            jax.ShapeDtypeStruct((rows, width), BF16),
            jax.ShapeDtypeStruct((rows, width), BF16),
            jax.ShapeDtypeStruct((width, rows), BF16),
            cache,
            cache,
        ],
        in_specs=in_specs,
        out_specs=[
            pl.BlockSpec((tile, width), lambda i: (i, 0)),
            pl.BlockSpec((tile, width), lambda i: (i, 0)),
            pl.BlockSpec((width, tile), lambda i: (0, i)),
            cache_spec,
            cache_spec,
        ],
        input_output_aliases=alias,
        compiler_params=pltpu.CompilerParams(vmem_limit_bytes=40 * MIB),
        cost_estimate=pl.CostEstimate(flops=2 * rows * model * 3 * width, bytes_accessed=rows * model * 2, transcendentals=0),
    )(*args)


def attn_kernel(n, heads, dim, parts, q_ref, *refs):
    kv = [(refs[2 * p], refs[2 * p + 1]) for p in range(parts)]
    out_ref, o_buf, local_sem, send_sem, recv_sem = refs[2 * parts :]
    me = lax.axis_index("cp")
    rows, width = q_ref.shape
    block = rows // n
    scale = LOG2E * dim**-0.5
    greet_all(n, me)

    def chunk(queries, k_ref, vt_ref, start, size, carry, masked):
        scores = []
        for h in range(heads):
            k = k_ref[pl.ds(start, size), h * dim : (h + 1) * dim]
            s = lax.dot_general(k, queries[h], (((1,), (1,)), ((), ())), preferred_element_type=F32)
            if masked:
                row = lax.broadcasted_iota(jnp.int32, s.shape, 0)
                col = lax.broadcasted_iota(jnp.int32, s.shape, 1)
                s = jnp.where(row <= col, s, -jnp.inf)
            scores.append(s)
        out = []
        for h in range(heads):
            m, l, acc = carry[h]
            s = scores[h]
            m_new = jnp.maximum(m, jnp.max(s, axis=0, keepdims=True))
            a = jnp.exp2((m - m_new) * scale)
            p = jnp.exp2((s - m_new) * scale)
            l = l * a + jnp.sum(p, axis=0, keepdims=True)
            vt = vt_ref[h * dim : (h + 1) * dim, pl.ds(start, size)]
            acc = acc * a + jnp.dot(vt, p.astype(BF16), preferred_element_type=F32)
            out.append((m_new, l, acc))
        return tuple(out)

    def owner(b):
        return b if parts == 1 else n - 1 - b

    def own_copy(b):
        src = o_buf.at[pl.ds(pl.multiple_of(b * block, block), block), :]
        cols = pl.ds(pl.multiple_of(me * width, width), width)
        return pltpu.make_async_copy(src, out_ref.at[:, cols], local_sem)

    def copy(b, source):
        src = o_buf.at[pl.ds(pl.multiple_of(b * block, block), block), :]
        cols = pl.ds(pl.multiple_of(source * width, width), width)
        return pltpu.make_async_remote_copy(
            src_ref=src, dst_ref=out_ref.at[:, cols], send_sem=send_sem.at[b], recv_sem=recv_sem.at[source],
            device_id={"cp": owner(b)}, device_id_type=MESH,
        )

    tiles = rows // TQ

    def tile(i, _):
        t = lax.rem(i + me, tiles)
        at = pl.multiple_of(t * TQ, TQ)
        queries = [q_ref[pl.ds(at, TQ), h * dim : (h + 1) * dim] for h in range(heads)]
        carry = tuple(
            (jnp.full((1, TQ), -jnp.inf, F32), jnp.zeros((1, TQ), F32), jnp.zeros((dim, TQ), F32)) for _ in range(heads)
        )
        if parts == 2:
            k_ref, vt_ref = kv[0]
            carry = lax.fori_loop(
                0, k_ref.shape[0] // TK,
                lambda j, c: chunk(queries, k_ref, vt_ref, pl.multiple_of(j * TK, TK), TK, c, False), carry,
            )
        k_last, vt_last = kv[-1]
        per = TK // TQ
        full = t // per
        carry = lax.fori_loop(
            0, full, lambda j, c: chunk(queries, k_last, vt_last, pl.multiple_of(j * TK, TK), TK, c, False), carry
        )
        carry = lax.fori_loop(
            full * per, t, lambda j, c: chunk(queries, k_last, vt_last, pl.multiple_of(j * TQ, TQ), TQ, c, False), carry
        )
        carry = chunk(queries, k_last, vt_last, at, TQ, carry, True)
        for h in range(heads):
            m, l, acc = carry[h]
            o_buf[pl.ds(at, TQ), h * dim : (h + 1) * dim] = (acc / l).T.astype(BF16)
        for j in range(TQ // block):
            b = t * (TQ // block) + j

            @pl.when(owner(b) == me)
            def _():
                own_copy(b).start()

            @pl.when(owner(b) != me)
            def _():
                copy(b, me).start()

        return 0

    lax.fori_loop(0, tiles, tile, 0)
    own_copy(owner(me)).wait()
    for d in range(1, n):
        other = lax.rem(me + d, n)
        copy(owner(other), me).wait_send()
        copy(owner(other), other).wait_recv()


def attention(q, kv, n, heads, dim, collective_id):
    rows, width = q.shape
    block = rows // n
    args = [q] + [a for pair in kv for a in pair]
    pairs = rows * rows * (2 * len(kv) - 1) // 2
    return pl.pallas_call(
        functools.partial(attn_kernel, n, heads, dim, len(kv)),
        name="attn",
        out_shape=jax.ShapeDtypeStruct((block, n * width), BF16),
        in_specs=[pl.BlockSpec(memory_space=pltpu.VMEM)] * len(args),
        out_specs=pl.BlockSpec(memory_space=pl.ANY),
        scratch_shapes=[
            pltpu.VMEM((rows, width), BF16),
            pltpu.SemaphoreType.DMA,
            pltpu.SemaphoreType.DMA((n,)),
            pltpu.SemaphoreType.DMA((n,)),
        ],
        compiler_params=pltpu.CompilerParams(
            vmem_limit_bytes=48 * MIB, collective_id=collective_id, has_side_effects=True
        ),
        cost_estimate=pl.CostEstimate(flops=4 * pairs * width, bytes_accessed=rows * width * 8, transcendentals=pairs * heads),
    )(*args)


def block_kernel(out_steps, x_ref, oa_ref, ob_ref, wo_ref, gain_ref, wg_ref, wu_ref, wd_ref, y_ref, acc, normed):
    i = pl.program_id(0)
    last = pl.num_programs(0) - 1

    @pl.when(i < out_steps)
    def _():
        o = jnp.concatenate([oa_ref[...], ob_ref[...]], axis=0)
        part = jnp.dot(o, wo_ref[0], preferred_element_type=F32)

        @pl.when(i == 0)
        def _():
            acc[...] = part

        @pl.when(i > 0)
        def _():
            acc[...] += part

        @pl.when(i == out_steps - 1)
        def _():
            x = (x_ref[...].astype(F32) + acc[...]).astype(BF16)
            normed[...] = rms_norm(x, gain_ref[...])
            acc[...] = x.astype(F32)

    @pl.when(i >= out_steps)
    def _():
        h = normed[...]
        gate = jnp.dot(h, wg_ref[0], preferred_element_type=F32)
        up = jnp.dot(h, wu_ref[0], preferred_element_type=F32)
        act = (jax.nn.silu(gate) * up).astype(BF16)
        acc[...] += jnp.dot(act, wd_ref[0], preferred_element_type=F32)

    @pl.when(i == last)
    def _():
        y_ref[...] = acc[...].astype(BF16)


def block_tail(x, o_a, o_b, w_out, gain, w_gate, w_up, w_down, layer):
    rows, model = x.shape
    half, inner = o_a.shape
    ffn = w_gate.shape[2]
    out_steps = 4
    step = inner // out_steps
    w_out = w_out.reshape(w_out.shape[0], inner, model)
    whole = pl.BlockSpec((rows, model), lambda i: (0, 0))
    out_at = lambda i: jnp.minimum(i, out_steps - 1)
    mlp_at = lambda i: jnp.maximum(i - out_steps, 0)
    return pl.pallas_call(
        functools.partial(block_kernel, out_steps),
        name="tail",
        grid=(out_steps + ffn // TF,),
        out_shape=jax.ShapeDtypeStruct((rows, model), BF16),
        in_specs=[
            whole,
            pl.BlockSpec((half, step), lambda i: (0, out_at(i))),
            pl.BlockSpec((half, step), lambda i: (0, out_at(i))),
            pl.BlockSpec((1, step, model), lambda i: (layer, out_at(i), 0)),
            pl.BlockSpec((1, model), lambda i: (0, 0)),
            pl.BlockSpec((1, model, TF), lambda i: (layer, 0, mlp_at(i))),
            pl.BlockSpec((1, model, TF), lambda i: (layer, 0, mlp_at(i))),
            pl.BlockSpec((1, TF, model), lambda i: (layer, mlp_at(i), 0)),
        ],
        out_specs=whole,
        scratch_shapes=[pltpu.VMEM((rows, model), F32), pltpu.VMEM((rows, model), BF16)],
        compiler_params=pltpu.CompilerParams(vmem_limit_bytes=60 * MIB),
        cost_estimate=pl.CostEstimate(
            flops=2 * rows * model * (inner + 3 * ffn), bytes_accessed=2 * model * (inner + 3 * ffn), transcendentals=rows * ffn
        ),
    )(x, o_a, o_b, w_out, gain[layer : layer + 1], w_gate, w_up, w_down)


def solution(mesh):
    cp_size = mesh.shape["cp"]
    row_spec = P(("req", "cp"), None)
    pos_spec = P(("req", "cp"))
    rep_spec = P()
    cache_spec = P(None, "req", "cp", None)

    def per_device(hidden, positions, gain_attn, gain_mlp, w_query, w_key, w_value, w_out, w_gate, w_up, w_down):
        num_layers, model, all_heads, dim = w_query.shape
        heads = all_heads // cp_size
        width = heads * dim
        rows = hidden.shape[0]
        block = rows // 2
        half = cp_size * block
        cache_shape = (num_layers, 2 * half, heads, dim)

        pos_all = share(positions.reshape(rows // 128, 128), cp_size).reshape(cp_size, rows)
        pos_nat = jnp.concatenate([pos_all[:, :block].reshape(-1), pos_all[::-1, block:].reshape(-1)])
        cos, sin = rope_tables(pos_nat, dim)
        caches = None
        for layer in range(num_layers):
            normed = rms_norm(hidden, gain_attn[layer])
            me, normed = lax.optimization_barrier((lax.axis_index("cp"), normed))
            h_a = lax.all_gather(normed[:block], "cp", tiled=True)
            h_b = lax.all_gather(normed[block:], "cp", tiled=True)

            def mine(w):
                own = lax.dynamic_slice(w, (layer, 0, me * heads, 0), (1, model, heads, dim))
                return own.reshape(model, width)

            w_all = jnp.concatenate([mine(w_query), mine(w_key), mine(w_value)], axis=1)
            q_a, k_a, vt_a, *caches = qkv(h_a, w_all, cos, sin, caches, cache_shape, layer, 0, False, block)
            o_a = attention(q_a, [(k_a, vt_a)], cp_size, heads, dim, 1)
            q_b, k_b, vt_b, *caches = qkv(h_b, w_all, cos, sin, caches, cache_shape, layer, cp_size, True, block)
            o_b = attention(q_b, [(k_a, vt_a), (k_b, vt_b)], cp_size, heads, dim, 2)
            hidden = block_tail(hidden, o_a, o_b, w_out, gain_mlp, w_gate, w_up, w_down, layer)
        return hidden, caches[0], caches[1]

    in_specs = (row_spec, pos_spec) + (rep_spec,) * 9
    return jax.shard_map(per_device, mesh=mesh, in_specs=in_specs, out_specs=(row_spec, cache_spec, cache_spec), check_vma=False)
```

```python
import functools

import jax
import jax.numpy as jnp
from jax import lax
from jax.experimental import pallas as pl
from jax.experimental.pallas import tpu as pltpu
from jax.sharding import PartitionSpec as P

NORM_EPS = 1e-5
ROPE_BASE = 10000.0
LOG2E = 1.4426950408889634
MESH = pl.DeviceIdType.MESH
MIB = 1024 * 1024
TQ = 512
TK = 1024
TF = 1024
BF16, F32 = jnp.bfloat16, jnp.float32


def rms_norm(values, gain_vec):
    wide_vals = values.astype(F32)
    inv_rms = lax.rsqrt(jnp.mean(wide_vals * wide_vals, axis=-1, keepdims=True) + NORM_EPS)
    return (wide_vals * inv_rms * gain_vec.astype(F32)).astype(BF16)


def greet_all(n, me):
    barrier = pltpu.get_barrier_semaphore()
    for d in range(1, n):
        pl.semaphore_signal(barrier, inc=1, device_id={"cp": lax.rem(me + d, n)}, device_id_type=MESH)
    pl.semaphore_wait(barrier, n - 1)


def front_kernel(
    n, heads, dim, layer, first, x_ref, gain_ref, *refs
):
    if first:
        pos_ref, freq_ref, *refs = refs
        wq_ref, wk_ref, wv_ref, oa_ref, ob_ref, k_ref, v_ref, cos_ref, sin_ref, *refs = refs
        pos_buf, pos_send, pos_recv, *refs = refs
    else:
        cos_ref, sin_ref, wq_ref, wk_ref, wv_ref, oa_ref, ob_ref, k_ref, v_ref, *refs = refs
    h_buf, w_raw, w_buf, q_ref, vt_ref, o_buf, m_st, l_st, acc_st, *sems = refs
    w_sem, recv_sem, own_sem, fwd_sem, relay_sem, o_local, o_send, o_recv = sems
    block, model = h_buf.shape[2:]
    rows = n * block
    piece = block // 2
    width = heads * dim
    scale = LOG2E * dim**-0.5
    chips = n // 2
    me = lax.axis_index("cp")
    chip, core = me // 2, lax.rem(me, 2)

    def at(step, k):
        return 2 * lax.rem(chip + step, chips) + k

    right, left, opp, partner = at(1, core), at(chips - 1, core), at(2, core), at(0, 1 - core)
    sources = (left, right, opp)

    def remote(s, origin, p, target, sem):
        part = h_buf.at[s, origin, pl.ds(p * piece, piece)]
        return pltpu.make_async_remote_copy(
            src_ref=part, dst_ref=part, send_sem=sem, recv_sem=recv_sem.at[s, origin, p],
            device_id={"cp": target}, device_id_type=MESH,
        )

    own_sends = [(right, 0), (left, 1), (right, 1), (left, 0), (partner, 0), (partner, 1)]

    def send_own(s):
        for j, (target, p) in enumerate(own_sends):
            remote(s, me, p, target, own_sem.at[s, j]).start()

    def arrived(s, origin, p):
        remote(s, origin, p, partner, own_sem.at[s, 0]).wait_recv()

    def relay(s, j, p):
        return remote(s, sources[j], p, partner, relay_sem.at[s, j, p])

    def forward(s, way):
        return remote(s, (left, right)[way], way, (right, left)[way], fwd_sem.at[s, way])

    def pass_on(s):
        for way in range(2):
            arrived(s, (left, right)[way], way)
            forward(s, way).start()
            relay(s, way, way).start()

    def receive(s, k):
        @pl.when(k == 0)
        def _():
            for p in range(2):
                arrived(s, partner, p)

        @pl.when(k == 1)
        def _():
            for way in range(2):
                arrived(s, (left, right)[way], 1 - way)
                relay(s, way, 1 - way).start()
            for p in range(2):
                arrived(s, at(chips - 1, 1 - core), p)

        @pl.when(k == 2)
        def _():
            for p in range(2):
                arrived(s, at(1, 1 - core), p)

        @pl.when(k == 3)
        def _():
            for p in range(2):
                arrived(s, opp, p)
                relay(s, 2, p).start()
            for p in range(2):
                arrived(s, at(2, 1 - core), p)

    def place(s, d):
        return pl.multiple_of(d * block if s == 0 else rows + (n - 1 - d) * block, block)

    def project(s, c):
        h = h_buf[s, pl.ds(2 * c, 2)].reshape(2 * block, model)
        at0 = pl.multiple_of(2 * c * block if s == 0 else rows + (n - 2 - 2 * c) * block, 2 * block)
        both = pl.ds(at0, 2 * block)
        cos, sin = cos_ref[both, :], sin_ref[both, :]

        def natural(y):
            return y if s == 0 else jnp.concatenate([y[block:], y[:block]], axis=0)

        def rope(x):
            return x * cos + pltpu.roll(x, dim // 2, 1) * sin

        ys = [
            natural(jnp.dot(h, w_buf[:, j * width : (j + 1) * width], preferred_element_type=F32)) for j in (1, 2, 0)
        ]
        for g in range(heads):
            lo, hi = g * dim, (g + 1) * dim
            k_ref[both, lo:hi] = rope(ys[0][:, lo:hi]).astype(BF16)
            q_ref[both, lo:hi] = rope(ys[2][:, lo:hi]).astype(BF16)
        v_ref[both, :] = ys[1].astype(BF16)
        vt_ref[:, both] = ys[1].T.astype(BF16)

    def chunk(queries, start, size, carry, masked):
        scores = []
        for g in range(heads):
            k = k_ref[pl.ds(start, size), g * dim : (g + 1) * dim]
            s = lax.dot_general(k, queries[g], (((1,), (1,)), ((), ())), preferred_element_type=F32)
            if masked:
                row = lax.broadcasted_iota(jnp.int32, s.shape, 0)
                col = lax.broadcasted_iota(jnp.int32, s.shape, 1)
                s = jnp.where(row <= col, s, -jnp.inf)
            scores.append(s)
        out = []
        for g in range(heads):
            m, l, acc = carry[g]
            s = scores[g]
            m_new = jnp.maximum(m, jnp.max(s, axis=0, keepdims=True))
            a = jnp.exp2((m - m_new) * scale)
            p = jnp.exp2((s - m_new) * scale)
            l = l * a + jnp.sum(p, axis=0, keepdims=True)
            vt = vt_ref[g * dim : (g + 1) * dim, pl.ds(start, size)]
            acc = acc * a + jnp.dot(vt, p.astype(BF16), preferred_element_type=F32)
            out.append((m_new, l, acc))
        return tuple(out)

    def chunks(queries, lo, hi, base, size, carry):
        return lax.fori_loop(
            lo, hi, lambda j, c: chunk(queries, pl.multiple_of(base + j * size, size), size, c, False), carry
        )

    def queries_at(start):
        return [q_ref[pl.ds(start, TQ), g * dim : (g + 1) * dim] for g in range(heads)]

    def fresh():
        return tuple(
            (jnp.full((1, TQ), -jnp.inf, F32), jnp.zeros((1, TQ), F32), jnp.zeros((dim, TQ), F32)) for _ in range(heads)
        )

    def finish(t, base, carry):
        start = pl.multiple_of(base + t * TQ, TQ)
        queries = queries_at(start)
        per = TK // TQ
        full = t // per
        carry = chunks(queries, 0, full, base, TK, carry)
        carry = chunks(queries, full * per, t, base, TQ, carry)
        carry = chunk(queries, start, TQ, carry, True)
        for g in range(heads):
            m, l, acc = carry[g]
            o_buf[pl.ds(start, TQ), g * dim : (g + 1) * dim] = (acc / l).T.astype(BF16)

    outs = (oa_ref, ob_ref)

    def own_result(s):
        cols = pl.ds(pl.multiple_of(me * width, width), width)
        return pltpu.make_async_copy(o_buf.at[pl.ds(place(s, me), block), :], outs[s].at[:, cols], o_local.at[s])

    def result(s, d, source):
        cols = pl.ds(pl.multiple_of(source * width, width), width)
        return pltpu.make_async_remote_copy(
            src_ref=o_buf.at[pl.ds(place(s, d), block), :], dst_ref=outs[s].at[:, cols],
            send_sem=o_send.at[s, d], recv_sem=o_recv.at[s, source],
            device_id={"cp": d}, device_id_type=MESH,
        )

    loads = [
        pltpu.make_async_copy(w.at[layer, :, me], w_raw.at[j], w_sem.at[j]) for j, w in enumerate((wq_ref, wk_ref, wv_ref))
    ]
    for load in loads:
        load.start()
    for s in range(2):
        h_buf[s, me] = rms_norm(x_ref[s * block : (s + 1) * block, :], gain_ref[...])
    greet_all(n, me)
    if first:
        def pos_copy(d, slot):
            return pltpu.make_async_remote_copy(
                src_ref=pos_ref, dst_ref=pos_buf.at[slot], send_sem=pos_send.at[d], recv_sem=pos_recv.at[slot],
                device_id={"cp": lax.rem(me + d, n)}, device_id_type=MESH,
            )

        for d in range(1, n):
            pos_copy(d, me).start()
    send_own(0)
    if first:
        pos_buf[me] = pos_ref[...]
    for j in range(3):
        loads[j].wait()

        def unpack(i, _, j=j):
            part = pl.ds(pl.multiple_of(i * 256, 256), 256)
            w = w_raw[j, part]
            for g in range(heads):
                w_buf[part, j * width + g * dim : j * width + (g + 1) * dim] = w[:, g, :]
            return 0

        lax.fori_loop(0, model // 256, unpack, 0)
    pass_on(0)
    send_own(1)
    if first:
        for d in range(1, n):
            pos_copy(d, me).wait_send()
            pos_copy(d, lax.rem(me + d, n)).wait_recv()
        sign = jnp.where(lax.broadcasted_iota(jnp.int32, (1, dim), 1) < dim // 2, -1.0, 1.0).astype(F32)

        def tables(s, d):
            for j in range(block // 128):
                pos = pos_buf[d, s * (block // 128) + j : s * (block // 128) + j + 1, :].astype(F32)
                angles = jnp.broadcast_to(pos, (128, 128)).T * freq_ref[...]
                part = pl.ds(pl.multiple_of(place(s, d) + j * 128, 128), 128)
                cos_ref[part, :] = jnp.cos(angles)
                sin_ref[part, :] = jnp.sin(angles) * sign

    def half(s):
        def step(k, _):
            c = lax.rem(chip + jnp.where(k == 0, 0, jnp.where(k == 1, chips - 1, k - 1)), chips)
            if first:
                for d in range(2):
                    tables(s, 2 * c + d)
            receive(s, k)
            project(s, c)
            if s == 1:
                t = chips - 1 - c
                queries = queries_at(pl.multiple_of(rows + t * TQ, TQ))
                carry = chunks(queries, 0, rows // TK, 0, TK, fresh())
                for g in range(heads):
                    m_st[t, g], l_st[t, g], acc_st[t, g] = carry[g]
            return 0

        lax.fori_loop(0, chips, step, 0)

    half(0)

    def tile_a(t, _):
        finish(t, 0, fresh())
        return 0

    lax.fori_loop(0, chips, tile_a, 0)
    pass_on(1)
    own_result(0).start()
    for d in range(1, n):
        other = lax.rem(me + d, n)
        result(0, other, me).start()
    half(1)

    def tile_b(i, _):
        t = lax.rem(i + chip, chips)
        finish(t, rows, tuple((m_st[t, g], l_st[t, g], acc_st[t, g]) for g in range(heads)))
        for j in range(2):
            d = n - 1 - (2 * t + j)

            @pl.when(d == me)
            def _():
                own_result(1).start()

            @pl.when(d != me)
            def _():
                result(1, d, me).start()

        return 0

    lax.fori_loop(0, chips, tile_b, 0)
    for s in range(2):
        for j, (target, p) in enumerate(own_sends):
            remote(s, me, p, target, own_sem.at[s, j]).wait_send()
        for way in range(2):
            forward(s, way).wait_send()
        for j in range(3):
            for p in range(2):
                relay(s, j, p).wait_send()
        own_result(s).wait()
        for d in range(1, n):
            other = lax.rem(me + d, n)
            result(s, other, me).wait_send()
            result(s, other, other).wait_recv()


def front(x, gain, tables, w_query, w_key, w_value, n, layer):
    first = len(tables) == 2 and tables[0].dtype == jnp.int32
    rows, model = x.shape
    num_layers, _, all_heads, dim = w_query.shape
    heads = all_heads // n
    width = heads * dim
    block = rows // 2
    seq = n * rows
    vmem = pl.BlockSpec(memory_space=pltpu.VMEM)
    hbm = pl.BlockSpec(memory_space=pl.ANY)
    chips = n // 2
    out = jax.ShapeDtypeStruct((block, all_heads * dim), BF16)
    kv = jax.ShapeDtypeStruct((seq, width), BF16)
    table = jax.ShapeDtypeStruct((seq, dim), F32)
    dma = pltpu.SemaphoreType.DMA
    pos_scratch = [pltpu.VMEM((n,) + tables[0].shape, jnp.int32), dma((n,)), dma((n,))] if first else []
    by_head = [w.reshape(num_layers, model, n, heads, dim) for w in (w_query, w_key, w_value)]
    return pl.pallas_call(
        functools.partial(front_kernel, n, heads, dim, layer, first),
        name="front",
        out_shape=[out, out, kv, kv] + ([table, table] if first else []),
        in_specs=[vmem, vmem, vmem, vmem, hbm, hbm, hbm],
        out_specs=[hbm, hbm, vmem, vmem] + ([vmem, vmem] if first else []),
        scratch_shapes=pos_scratch
        + [
            pltpu.VMEM((2, n, block, model), BF16),
            pltpu.VMEM((3, model, heads, dim), BF16),
            pltpu.VMEM((model, 3 * width), BF16),
            pltpu.VMEM((seq, width), BF16),
            pltpu.VMEM((width, seq), BF16),
            pltpu.VMEM((seq, width), BF16),
            pltpu.VMEM((chips, heads, 1, TQ), F32),
            pltpu.VMEM((chips, heads, 1, TQ), F32),
            pltpu.VMEM((chips, heads, dim, TQ), F32),
            dma((3,)),
            dma((2, n, 2)),
            dma((2, 6)),
            dma((2, 2)),
            dma((2, 3, 2)),
            dma((2,)),
            dma((2, n)),
            dma((2, n)),
        ],
        compiler_params=pltpu.CompilerParams(vmem_limit_bytes=62 * MIB, collective_id=layer + 1, has_side_effects=True),
        cost_estimate=pl.CostEstimate(flops=6 * seq * model * width + 2 * seq * seq * width, bytes_accessed=seq * model * 2, transcendentals=seq * seq * heads // 2),
    )(x, gain[layer : layer + 1], *tables, *by_head)


def block_kernel(out_steps, aliased, x_ref, oa_ref, ob_ref, wo_ref, gain_ref, wg_ref, wu_ref, wd_ref, k_ref, v_ref, *refs):
    y_ref, kc_ref, vc_ref, acc, normed = refs[2:] if aliased else refs
    i = pl.program_id(0)
    last = pl.num_programs(0) - 1

    @pl.when(i < out_steps)
    def _():
        o = jnp.concatenate([oa_ref[...], ob_ref[...]], axis=0)
        part = jnp.dot(o, wo_ref[0], preferred_element_type=F32)

        @pl.when(i == 0)
        def _():
            acc[...] = part

        @pl.when(i > 0)
        def _():
            acc[...] += part

        @pl.when(i == out_steps - 1)
        def _():
            x = (x_ref[...].astype(F32) + acc[...]).astype(BF16)
            normed[...] = rms_norm(x, gain_ref[...])
            acc[...] = x.astype(F32)

    @pl.when(i >= out_steps)
    def _():
        h = normed[...]
        gate = jnp.dot(h, wg_ref[0], preferred_element_type=F32)
        up = jnp.dot(h, wu_ref[0], preferred_element_type=F32)
        act = (jax.nn.silu(gate) * up).astype(BF16)
        acc[...] += jnp.dot(act, wd_ref[0], preferred_element_type=F32)
        heads, dim = kc_ref.shape[2:]
        for src, dst in ((k_ref, kc_ref), (v_ref, vc_ref)):
            flat = src[...].astype(F32)
            dst[0] = jnp.stack([flat[:, g * dim : (g + 1) * dim] for g in range(heads)], axis=1).astype(BF16)

    @pl.when(i == last)
    def _():
        y_ref[...] = acc[...].astype(BF16)


def block_tail(x, o_a, o_b, k, v, caches, cache_shape, w_out, gain, w_gate, w_up, w_down, layer):
    rows, model = x.shape
    half, inner = o_a.shape
    ffn = w_gate.shape[2]
    out_steps = 4
    step = inner // out_steps
    heads, dim = cache_shape[2:]
    part = k.shape[0] // (ffn // TF)
    w_out = w_out.reshape(w_out.shape[0], inner, model)
    whole = pl.BlockSpec((rows, model), lambda i: (0, 0))
    out_at = lambda i: jnp.minimum(i, out_steps - 1)
    mlp_at = lambda i: jnp.maximum(i - out_steps, 0)
    cache = jax.ShapeDtypeStruct(cache_shape, BF16)
    cache_spec = pl.BlockSpec((1, part, heads, dim), lambda i: (layer, mlp_at(i), 0, 0))
    kv_spec = pl.BlockSpec((part, heads * dim), lambda i: (mlp_at(i), 0))
    return pl.pallas_call(
        functools.partial(block_kernel, out_steps, bool(caches)),
        name="tail",
        grid=(out_steps + ffn // TF,),
        out_shape=[jax.ShapeDtypeStruct((rows, model), BF16), cache, cache],
        in_specs=[
            whole,
            pl.BlockSpec((half, step), lambda i: (0, out_at(i))),
            pl.BlockSpec((half, step), lambda i: (0, out_at(i))),
            pl.BlockSpec((1, step, model), lambda i: (layer, out_at(i), 0)),
            pl.BlockSpec((1, model), lambda i: (0, 0)),
            pl.BlockSpec((1, model, TF), lambda i: (layer, 0, mlp_at(i))),
            pl.BlockSpec((1, model, TF), lambda i: (layer, 0, mlp_at(i))),
            pl.BlockSpec((1, TF, model), lambda i: (layer, mlp_at(i), 0)),
            kv_spec,
            kv_spec,
        ]
        + [pl.BlockSpec(memory_space=pl.ANY)] * len(caches),
        out_specs=[whole, cache_spec, cache_spec],
        scratch_shapes=[pltpu.VMEM((rows, model), F32), pltpu.VMEM((rows, model), BF16)],
        input_output_aliases={10: 1, 11: 2} if caches else {},
        compiler_params=pltpu.CompilerParams(vmem_limit_bytes=60 * MIB),
        cost_estimate=pl.CostEstimate(
            flops=2 * rows * model * (inner + 3 * ffn), bytes_accessed=2 * model * (inner + 3 * ffn), transcendentals=rows * ffn
        ),
    )(x, o_a, o_b, w_out, gain[layer : layer + 1], w_gate, w_up, w_down, k, v, *caches)


def solution(mesh):
    cp_size = mesh.shape["cp"]
    row_spec = P(("req", "cp"), None)
    pos_spec = P(("req", "cp"))
    rep_spec = P()
    cache_spec = P(None, "req", "cp", None)

    def per_device(hidden, positions, gain_attn, gain_mlp, w_query, w_key, w_value, w_out, w_gate, w_up, w_down):
        num_layers, model, all_heads, dim = w_query.shape
        rows = hidden.shape[0]
        cache_shape = (num_layers, cp_size * rows, all_heads // cp_size, dim)
        inv_freq = ROPE_BASE ** (-jnp.arange(0, dim, 2, dtype=F32) / dim)
        tables = [positions.reshape(rows // 128, 128), jnp.concatenate([inv_freq, inv_freq])[None]]
        caches = []
        for layer in range(num_layers):
            o_a, o_b, k, v, *new = front(hidden, gain_attn, tables, w_query, w_key, w_value, cp_size, layer)
            tables = new or tables
            hidden, *caches = block_tail(
                hidden, o_a, o_b, k, v, caches, cache_shape, w_out, gain_mlp, w_gate, w_up, w_down, layer
            )
        return hidden, caches[0], caches[1]

    in_specs = (row_spec, pos_spec) + (rep_spec,) * 9
    return jax.shard_map(per_device, mesh=mesh, in_specs=in_specs, out_specs=(row_spec, cache_spec, cache_spec), check_vma=False)
```

```python
import functools

import jax
import jax.numpy as jnp
from jax import lax
from jax.experimental import pallas as pl
from jax.experimental.pallas import tpu as pltpu
from jax.sharding import PartitionSpec as P

NORM_EPS = 1e-5
ROPE_BASE = 10000.0
LOG2E = 1.4426950408889634
MESH = pl.DeviceIdType.MESH
MIB = 1024 * 1024
TQ = 512
TK = 1024
SLOTS = 7
TF = 512
BF16, F32 = jnp.bfloat16, jnp.float32


def rms_norm(values, gain_vec):
    wide_vals = values.astype(F32)
    inv_rms = lax.rsqrt(jnp.mean(wide_vals * wide_vals, axis=-1, keepdims=True) + NORM_EPS)
    return (wide_vals * inv_rms * gain_vec.astype(F32)).astype(BF16)


def greet_all(n, me):
    barrier = pltpu.get_barrier_semaphore()
    for d in range(1, n):
        pl.semaphore_signal(barrier, inc=1, device_id={"cp": lax.rem(me + d, n)}, device_id_type=MESH)
    pl.semaphore_wait(barrier, n - 1)


def front_kernel(
    n, heads, dim, layer, first, x_ref, gain_ref, *refs
):
    if first:
        pos_ref, freq_ref, *refs = refs
        wq_ref, wk_ref, wv_ref, o_ref, k_ref, v_ref, cos_ref, sin_ref, *refs = refs
        pos_buf, pos_send, pos_recv, *refs = refs
    else:
        cos_ref, sin_ref, ha_ref, wq_ref, wk_ref, wv_ref, o_ref, k_ref, v_ref, ha_sem, *refs = refs
    h_buf, w_raw, w_buf, q_ref, vt_ref, o_buf, m_st, l_st, acc_st, *sems = refs
    w_sem, recv_sem, own_sem, fwd_sem, relay_sem, o_local, o_send, o_recv = sems
    block, model = h_buf.shape[2:]
    rows = n * block
    piece = block // 2
    width = heads * dim
    scale = LOG2E * dim**-0.5
    chips = n // 2
    me = lax.axis_index("cp")
    chip, core = me // 2, lax.rem(me, 2)

    def at(step, k):
        return 2 * lax.rem(chip + step, chips) + k

    right, left, opp, partner = at(1, core), at(chips - 1, core), at(2, core), at(0, 1 - core)
    sources = (left, right, opp)

    def remote(s, origin, p, target, sem):
        part = h_buf.at[s, origin, pl.ds(p * piece, piece)]
        return pltpu.make_async_remote_copy(
            src_ref=part, dst_ref=part, send_sem=sem, recv_sem=recv_sem.at[s, origin, p],
            device_id={"cp": target}, device_id_type=MESH,
        )

    own_sends = [(right, 0), (left, 1), (right, 1), (left, 0), (partner, 0), (partner, 1)]

    def send_own(s):
        for j, (target, p) in enumerate(own_sends):
            remote(s, me, p, target, own_sem.at[s, j]).start()

    def arrived(s, origin, p):
        remote(s, origin, p, partner, own_sem.at[s, 0]).wait_recv()

    def relay(s, j, p):
        return remote(s, sources[j], p, partner, relay_sem.at[s, j, p])

    def forward(s, way):
        return remote(s, (left, right)[way], way, (right, left)[way], fwd_sem.at[s, way])

    def pass_on(s):
        for way in range(2):
            arrived(s, (left, right)[way], way)
            forward(s, way).start()
            relay(s, way, way).start()

    def receive(s, k):
        @pl.when(k == 0)
        def _():
            for p in range(2):
                arrived(s, partner, p)

        @pl.when(k == 1)
        def _():
            for way in range(2):
                arrived(s, (left, right)[way], 1 - way)
                relay(s, way, 1 - way).start()
            for p in range(2):
                arrived(s, at(chips - 1, 1 - core), p)

        @pl.when(k == 2)
        def _():
            for p in range(2):
                arrived(s, at(1, 1 - core), p)

        @pl.when(k == 3)
        def _():
            for p in range(2):
                arrived(s, opp, p)
                relay(s, 2, p).start()
            for p in range(2):
                arrived(s, at(2, 1 - core), p)

    def ready(k):
        c = lax.rem(chip + (0, chips - 1, 1, 2)[k], chips)
        return pltpu.make_async_copy(ha_ref.at[pl.ds(2 * c, 2)], h_buf.at[0, pl.ds(2 * c, 2)], ha_sem.at[k])

    def place(s, d):
        return pl.multiple_of(d * block if s == 0 else rows + (n - 1 - d) * block, block)

    def project(s, c):
        h = h_buf[s, pl.ds(2 * c, 2)].reshape(2 * block, model)
        at0 = pl.multiple_of(2 * c * block if s == 0 else rows + (n - 2 - 2 * c) * block, 2 * block)
        both = pl.ds(at0, 2 * block)
        cos, sin = cos_ref[both, :], sin_ref[both, :]

        def natural(y):
            return y if s == 0 else jnp.concatenate([y[block:], y[:block]], axis=0)

        def rope(x):
            return x * cos + pltpu.roll(x, dim // 2, 1) * sin

        ys = [
            natural(jnp.dot(h, w_buf[:, j * width : (j + 1) * width], preferred_element_type=F32)) for j in (1, 2, 0)
        ]
        for g in range(heads):
            lo, hi = g * dim, (g + 1) * dim
            k_ref[both, lo:hi] = rope(ys[0][:, lo:hi]).astype(BF16)
            q_ref[both, lo:hi] = rope(ys[2][:, lo:hi]).astype(BF16)
        v_ref[both, :] = ys[1].astype(BF16)
        vt_ref[:, both] = ys[1].T.astype(BF16)

    def chunk(queries, start, size, carry, masked):
        scores = []
        for g in range(heads):
            k = k_ref[pl.ds(start, size), g * dim : (g + 1) * dim]
            s = lax.dot_general(k, queries[g], (((1,), (1,)), ((), ())), preferred_element_type=F32)
            if masked:
                row = lax.broadcasted_iota(jnp.int32, s.shape, 0)
                col = lax.broadcasted_iota(jnp.int32, s.shape, 1)
                s = jnp.where(row <= col, s, -jnp.inf)
            scores.append(s)
        out = []
        for g in range(heads):
            m, l, acc = carry[g]
            s = scores[g]
            m_new = jnp.maximum(m, jnp.max(s, axis=0, keepdims=True))
            a = jnp.exp2((m - m_new) * scale)
            p = jnp.exp2((s - m_new) * scale)
            l = l * a + jnp.sum(p, axis=0, keepdims=True)
            vt = vt_ref[g * dim : (g + 1) * dim, pl.ds(start, size)]
            acc = acc * a + jnp.dot(vt, p.astype(BF16), preferred_element_type=F32)
            out.append((m_new, l, acc))
        return tuple(out)

    def chunks(queries, lo, hi, base, size, carry):
        return lax.fori_loop(
            lo, hi, lambda j, c: chunk(queries, pl.multiple_of(base + j * size, size), size, c, False), carry
        )

    def queries_at(start):
        return [q_ref[pl.ds(start, TQ), g * dim : (g + 1) * dim] for g in range(heads)]

    def fresh():
        return tuple(
            (jnp.full((1, TQ), -jnp.inf, F32), jnp.zeros((1, TQ), F32), jnp.zeros((dim, TQ), F32)) for _ in range(heads)
        )

    def finish(t, base, carry):
        start = pl.multiple_of(base + t * TQ, TQ)
        queries = queries_at(start)
        per = TK // TQ
        full = t // per
        carry = chunks(queries, 0, full, base, TK, carry)
        carry = chunks(queries, full * per, t, base, TQ, carry)
        carry = chunk(queries, start, TQ, carry, True)
        for g in range(heads):
            m, l, acc = carry[g]
            o_buf[pl.ds(start, TQ), g * dim : (g + 1) * dim] = (acc / l).T.astype(BF16)

    outs = (o_ref.at[0], o_ref.at[1])
    gathers = (0, 1) if first else (1,)

    def own_result(s):
        cols = pl.ds(pl.multiple_of(me * width, width), width)
        return pltpu.make_async_copy(o_buf.at[pl.ds(place(s, me), block), :], outs[s].at[:, cols], o_local.at[s])

    def result(s, d, source):
        cols = pl.ds(pl.multiple_of(source * width, width), width)
        return pltpu.make_async_remote_copy(
            src_ref=o_buf.at[pl.ds(place(s, d), block), :], dst_ref=outs[s].at[:, cols],
            send_sem=o_send.at[s, d], recv_sem=o_recv.at[s, source],
            device_id={"cp": d}, device_id_type=MESH,
        )

    loads = [
        pltpu.make_async_copy(w.at[layer, :, me], w_raw.at[j], w_sem.at[j]) for j, w in enumerate((wq_ref, wk_ref, wv_ref))
    ]
    for load in loads:
        load.start()
    if not first:
        for k in range(chips):
            ready(k).start()
    for s in gathers:
        h_buf[s, me] = rms_norm(x_ref[s * block : (s + 1) * block, :], gain_ref[layer : layer + 1, :])
    greet_all(n, me)
    if first:
        def pos_copy(d, slot):
            return pltpu.make_async_remote_copy(
                src_ref=pos_ref, dst_ref=pos_buf.at[slot], send_sem=pos_send.at[d], recv_sem=pos_recv.at[slot],
                device_id={"cp": lax.rem(me + d, n)}, device_id_type=MESH,
            )

        for d in range(1, n):
            pos_copy(d, me).start()
    send_own(gathers[0])
    if first:
        pos_buf[me] = pos_ref[...]
    for j in range(3):
        loads[j].wait()

        def unpack(i, _, j=j):
            part = pl.ds(pl.multiple_of(i * 256, 256), 256)
            w = w_raw[j, part]
            for g in range(heads):
                w_buf[part, j * width + g * dim : j * width + (g + 1) * dim] = w[:, g, :]
            return 0

        lax.fori_loop(0, model // 256, unpack, 0)
    pass_on(gathers[0])
    if first:
        send_own(1)
        for d in range(1, n):
            pos_copy(d, me).wait_send()
            pos_copy(d, lax.rem(me + d, n)).wait_recv()
        sign = jnp.where(lax.broadcasted_iota(jnp.int32, (1, dim), 1) < dim // 2, -1.0, 1.0).astype(F32)

        def tables(s, d):
            for j in range(block // 128):
                pos = pos_buf[d, s * (block // 128) + j : s * (block // 128) + j + 1, :].astype(F32)
                angles = jnp.broadcast_to(pos, (128, 128)).T * freq_ref[...]
                part = pl.ds(pl.multiple_of(place(s, d) + j * 128, 128), 128)
                cos_ref[part, :] = jnp.cos(angles)
                sin_ref[part, :] = jnp.sin(angles) * sign

    def half(s):
        def step(k, _):
            c = lax.rem(chip + jnp.where(k == 0, 0, jnp.where(k == 1, chips - 1, k - 1)), chips)
            if first:
                for d in range(2):
                    tables(s, 2 * c + d)
            if s in gathers:
                receive(s, k)
            else:
                for j in range(chips):

                    @pl.when(k == j)
                    def _(j=j):
                        ready(j).wait()

            project(s, c)
            if s == 1:
                t = chips - 1 - c
                queries = queries_at(pl.multiple_of(rows + t * TQ, TQ))
                carry = chunks(queries, 0, rows // TK, 0, TK, fresh())
                for g in range(heads):
                    m_st[t, g], l_st[t, g], acc_st[t, g] = carry[g]
            return 0

        lax.fori_loop(0, chips, step, 0)

    half(0)

    def tile_a(t, _):
        finish(t, 0, fresh())
        return 0

    lax.fori_loop(0, chips, tile_a, 0)
    if first:
        pass_on(1)
    own_result(0).start()
    for d in range(1, n):
        other = lax.rem(me + d, n)
        result(0, other, me).start()
    half(1)

    def tile_b(i, _):
        t = lax.rem(i + chip, chips)
        finish(t, rows, tuple((m_st[t, g], l_st[t, g], acc_st[t, g]) for g in range(heads)))
        for j in range(2):
            d = n - 1 - (2 * t + j)

            @pl.when(d == me)
            def _():
                own_result(1).start()

            @pl.when(d != me)
            def _():
                result(1, d, me).start()

        return 0

    lax.fori_loop(0, chips, tile_b, 0)
    for s in gathers:
        for j, (target, p) in enumerate(own_sends):
            remote(s, me, p, target, own_sem.at[s, j]).wait_send()
        for way in range(2):
            forward(s, way).wait_send()
        for j in range(3):
            for p in range(2):
                relay(s, j, p).wait_send()
    for s in range(2):
        own_result(s).wait()
        for d in range(1, n):
            other = lax.rem(me + d, n)
            result(s, other, me).wait_send()
            result(s, other, other).wait_recv()


def front(x, gain, tables, w_query, w_key, w_value, n, layer):
    first = layer == 0
    rows, model = x.shape
    num_layers, _, all_heads, dim = w_query.shape
    heads = all_heads // n
    width = heads * dim
    block = rows // 2
    seq = n * rows
    vmem = pl.BlockSpec(memory_space=pltpu.VMEM)
    hbm = pl.BlockSpec(memory_space=pl.ANY)
    chips = n // 2
    out = jax.ShapeDtypeStruct((2, block, all_heads * dim), BF16)
    kv = jax.ShapeDtypeStruct((seq, width), BF16)
    table = jax.ShapeDtypeStruct((seq, dim), F32)
    dma = pltpu.SemaphoreType.DMA
    pos_scratch = [pltpu.VMEM((n,) + tables[0].shape, jnp.int32), dma((n,)), dma((n,))] if first else [dma((chips,))]
    by_head = [w.reshape(num_layers, model, n, heads, dim) for w in (w_query, w_key, w_value)]
    return pl.pallas_call(
        functools.partial(front_kernel, n, heads, dim, layer, first),
        name="front",
        out_shape=[out, kv, kv] + ([table, table] if first else []),
        in_specs=[vmem] * 4 + [hbm] * (3 if first else 4),
        out_specs=[hbm, vmem, vmem] + ([vmem, vmem] if first else []),
        scratch_shapes=pos_scratch
        + [
            pltpu.VMEM((2, n, block, model), BF16),
            pltpu.VMEM((3, model, heads, dim), BF16),
            pltpu.VMEM((model, 3 * width), BF16),
            pltpu.VMEM((seq, width), BF16),
            pltpu.VMEM((width, seq), BF16),
            pltpu.VMEM((seq, width), BF16),
            pltpu.VMEM((chips, heads, 1, TQ), F32),
            pltpu.VMEM((chips, heads, 1, TQ), F32),
            pltpu.VMEM((chips, heads, dim, TQ), F32),
            dma((3,)),
            dma((2, n, 2)),
            dma((2, 6)),
            dma((2, 2)),
            dma((2, 3, 2)),
            dma((2,)),
            dma((2, n)),
            dma((2, n)),
        ],
        compiler_params=pltpu.CompilerParams(vmem_limit_bytes=62 * MIB, collective_id=layer + 1, has_side_effects=True),
        cost_estimate=pl.CostEstimate(flops=6 * seq * model * width + 2 * seq * seq * width, bytes_accessed=seq * model * 2, transcendentals=seq * seq * heads // 2),
    )(x, gain, *tables, *by_head)


def mlp_parts(acc, normed, act, wg_ref, wu_ref, wd_ref, now):
    def gate_up(slot=0):
        h = normed[...]
        gate = jnp.dot(h, wg_ref[slot], preferred_element_type=F32)
        up = jnp.dot(h, wu_ref[slot], preferred_element_type=F32)
        act[now] = (jax.nn.silu(gate) * up).astype(BF16)

    def down(slot=0):
        acc[...] += jnp.dot(act[1 - now], wd_ref[slot], preferred_element_type=F32)

    return gate_up, down


def out_step(r, out_steps, layer, x_ref, o_ref, wo_ref, gain_ref, acc, normed):
    o = o_ref[...].reshape(acc.shape[0], o_ref.shape[2])
    part = jnp.dot(o, wo_ref[0], preferred_element_type=F32)

    @pl.when(r == 0)
    def _():
        acc[...] = part

    @pl.when(r > 0)
    def _():
        acc[...] += part

    @pl.when(r == out_steps - 1)
    def _():
        x = (x_ref[...].astype(F32) + acc[...]).astype(BF16)
        normed[...] = rms_norm(x, gain_ref[layer : layer + 1, :])
        acc[...] = x.astype(F32)


def last_kernel(
    out_steps, layer, x_ref, o_ref, wo_ref, gain_ref, wg_ref, wu_ref, wd_ref, *refs
):
    kv_refs = refs[: 2 * (layer + 1)]
    y_ref, kc_ref, vc_ref, acc, normed, act, mixed = refs[2 * (layer + 1) :]
    i = pl.program_id(0)
    last = pl.num_programs(0) - 1
    gate_up, down = mlp_parts(acc, normed, act, wg_ref, wu_ref, wd_ref, lax.rem(i, 2))

    @pl.when(i < out_steps)
    def _():
        out_step(i, out_steps, layer, x_ref, o_ref, wo_ref, gain_ref, acc, normed)

    def caches():
        dim = kc_ref.shape[2]
        for j, src in enumerate(kv_refs):
            count, heads = src.shape[0], src.shape[1] // dim
            for g in range(heads):
                mixed[j, pl.ds(g, count, stride=heads), :] = src[:, g * dim : (g + 1) * dim].astype(F32)
            (kc_ref, vc_ref)[j % 2][j // 2] = mixed[j].astype(BF16)

    @pl.when(i == out_steps)
    def _():
        gate_up()
        caches()

    @pl.when((i > out_steps) & (i < last))
    def _():
        down()
        gate_up()
        caches()

    @pl.when(i == last)
    def _():
        down()
        y_ref[...] = acc[...].astype(BF16)


def split_kernel(
    n, out_steps, layer, steps, x_ref, o_ref, wo_ref, gain_ref, next_gain_ref, wg_ref, wu_ref, wd_ref,
    y_ref, ha_ref, acc, normed, act, mine, wg_buf, wu_buf, wd_buf, w_sem, local_sem, recv_sem, own_sem, fwd_sem, relay_sem,
):
    i = pl.program_id(0)
    s, r = i // steps, lax.rem(i, steps)
    gate_up, down = mlp_parts(acc, normed, act, wg_buf, wu_buf, wd_buf, lax.rem(i, 2))
    slots, tf = wd_buf.shape[:2]
    slices = steps - out_steps - 1

    def load(kind, f):
        cols = pl.ds(pl.multiple_of(f * tf, tf), tf)
        src = (wg_ref.at[layer, :, cols], wu_ref.at[layer, :, cols], wd_ref.at[layer, cols])[kind]
        slot = lax.rem(f, slots)
        return pltpu.make_async_copy(src, (wg_buf, wu_buf, wd_buf)[kind].at[slot], w_sem.at[kind, slot])

    def slice_at(j):
        return jnp.where(s == 0, j, slices - 1 - j)

    def await_loads(kinds, f):
        @pl.when((s == 0) | (f < slices - slots))
        def _():
            for kind in kinds:
                load(kind, f).wait()

    def refill(kinds, f):
        after = jnp.where(s == 0, f + slots, f - slots)

        @pl.when((after >= 0) & (after < slices))
        def _():
            for kind in kinds:
                load(kind, after).start()

    f_up = slice_at(r - out_steps)
    f_down = slice_at(r - out_steps - 1)

    @pl.when(i == 0)
    def _():
        for f in range(slots):
            for kind in range(3):
                load(kind, f).start()
    piece = mine.shape[0] // 2
    chips = n // 2
    me = lax.axis_index("cp")
    chip, core = me // 2, lax.rem(me, 2)

    def at(step, k):
        return 2 * lax.rem(chip + step, chips) + k

    right, left, opp, partner = at(1, core), at(chips - 1, core), at(2, core), at(0, 1 - core)
    sources = (left, right, opp)
    own_sends = [(right, 0), (left, 1), (right, 1), (left, 0), (partner, 0), (partner, 1)]
    barrier = pltpu.get_barrier_semaphore()

    def remote(src, origin, p, target, sem):
        return pltpu.make_async_remote_copy(
            src_ref=src, dst_ref=ha_ref.at[origin, pl.ds(p * piece, piece)], send_sem=sem,
            recv_sem=recv_sem.at[origin, p], device_id={"cp": target}, device_id_type=MESH,
        )

    def held(origin, p):
        return ha_ref.at[origin, pl.ds(p * piece, piece)]

    def own(j):
        target, p = own_sends[j]
        return remote(mine.at[pl.ds(p * piece, piece)], me, p, target, own_sem.at[j])

    def keep():
        return pltpu.make_async_copy(mine, ha_ref.at[me], local_sem)

    def arrived(origin, p):
        remote(held(origin, p), origin, p, partner, own_sem.at[0]).wait_recv()

    def relay(j, p):
        return remote(held(sources[j], p), sources[j], p, partner, relay_sem.at[j, p])

    def forward(way):
        origin = (left, right)[way]
        return remote(held(origin, way), origin, way, (right, left)[way], fwd_sem.at[way])

    @pl.when(i == 0)
    def _():
        for d in range(1, n):
            pl.semaphore_signal(barrier, inc=1, device_id={"cp": lax.rem(me + d, n)}, device_id_type=MESH)
        pl.semaphore_wait(barrier, n - 1)

    @pl.when(i == steps + out_steps + 5)
    def _():
        for way in range(2):
            arrived((left, right)[way], way)
            forward(way).start()
            relay(way, way).start()

    @pl.when(i == steps + out_steps + 11)
    def _():
        for way in range(2):
            arrived((left, right)[way], 1 - way)
            relay(way, 1 - way).start()

    @pl.when(i == 2 * steps - 1)
    def _():
        for p in range(2):
            arrived(opp, p)
            relay(2, p).start()

    @pl.when(r < out_steps)
    def _():
        out_step(r, out_steps, layer, x_ref, o_ref, wo_ref, gain_ref, acc, normed)

    @pl.when((r >= out_steps) & (r < steps - 1))
    def _():
        await_loads((0, 1), f_up)

    @pl.when(r > out_steps)
    def _():
        await_loads((2,), f_down)

    @pl.when(r == out_steps)
    def _():
        gate_up(lax.rem(f_up, slots))

    @pl.when((r > out_steps) & (r < steps - 1))
    def _():
        down(lax.rem(f_down, slots))
        gate_up(lax.rem(f_up, slots))

    @pl.when(r == steps - 1)
    def _():
        down(lax.rem(f_down, slots))
        y_ref[...] = acc[...].astype(BF16)

    @pl.when((r >= out_steps) & (r < steps - 1))
    def _():
        refill((0, 1), f_up)

    @pl.when(r > out_steps)
    def _():
        refill((2,), f_down)

    @pl.when(i == steps - 1)
    def _():
        mine[...] = rms_norm(y_ref[...], next_gain_ref[layer + 1 : layer + 2, :])
        keep().start()
        for j in range(len(own_sends)):
            own(j).start()

    @pl.when(i == 2 * steps - 1)
    def _():
        keep().wait()
        for j in range(len(own_sends)):
            own(j).wait_send()
        for way in range(2):
            forward(way).wait_send()
        for j in range(3):
            for p in range(2):
                relay(j, p).wait_send()
        for origin in (partner, at(chips - 1, 1 - core), at(1, 1 - core), at(2, 1 - core)):
            for p in range(2):
                arrived(origin, p)


def tail_specs(layer, out_steps, slices, tf, model, step, r_of):
    out_at = lambda i: jnp.minimum(r_of(i), out_steps - 1)
    mlp_at = lambda i: jnp.clip(r_of(i) - out_steps, 0, slices - 1)
    down_at = lambda i: jnp.clip(r_of(i) - out_steps - 1, 0, slices - 1)
    w_out = pl.BlockSpec((1, step, model), lambda i: (layer, out_at(i), 0))
    mlp = [
        pl.BlockSpec((1, model, tf), lambda i: (layer, 0, mlp_at(i))),
        pl.BlockSpec((1, model, tf), lambda i: (layer, 0, mlp_at(i))),
        pl.BlockSpec((1, tf, model), lambda i: (layer, down_at(i), 0)),
    ]
    return out_at, mlp_at, w_out, mlp


def split_tail(x, o, n, w_out, gain, next_gain, w_gate, w_up, w_down, layer):
    rows, model = x.shape
    _, half, inner = o.shape
    ffn = w_gate.shape[2]
    out_steps, tf, slots = 2, TF, SLOTS
    slices = ffn // tf
    step = inner // out_steps
    steps = out_steps + slices + 1
    out_at, _, wo_spec, _ = tail_specs(layer, out_steps, slices, tf, model, step, lambda i: lax.rem(i, steps))
    hbm = pl.BlockSpec(memory_space=pl.ANY)
    part = pl.BlockSpec((half, model), lambda i: (i // steps, 0))
    full = pl.BlockSpec(gain.shape, lambda i: (0, 0))
    dma = pltpu.SemaphoreType.DMA
    return pl.pallas_call(
        functools.partial(split_kernel, n, out_steps, layer, steps),
        name="tail_split",
        grid=(2 * steps,),
        out_shape=[jax.ShapeDtypeStruct((rows, model), BF16), jax.ShapeDtypeStruct((n, half, model), BF16)],
        in_specs=[part, pl.BlockSpec((1, half, step), lambda i: (i // steps, 0, out_at(i))), wo_spec, full, full, hbm, hbm, hbm],
        out_specs=[part, pl.BlockSpec(memory_space=pl.ANY)],
        scratch_shapes=[
            pltpu.VMEM((half, model), F32),
            pltpu.VMEM((half, model), BF16),
            pltpu.VMEM((2, half, tf), BF16),
            pltpu.VMEM((half, model), BF16),
            pltpu.VMEM((slots, model, tf), BF16),
            pltpu.VMEM((slots, model, tf), BF16),
            pltpu.VMEM((slots, tf, model), BF16),
            dma((3, slots)),
            dma,
            dma((n, 2)),
            dma((6,)),
            dma((2,)),
            dma((3, 2)),
        ],
        compiler_params=pltpu.CompilerParams(vmem_limit_bytes=63 * MIB, collective_id=8 + layer, has_side_effects=True),
        cost_estimate=pl.CostEstimate(
            flops=2 * rows * model * (inner + 3 * ffn), bytes_accessed=4 * model * (inner + 3 * ffn), transcendentals=rows * ffn
        ),
    )(x, o, w_out.reshape(w_out.shape[0], inner, model), gain, next_gain, w_gate, w_up, w_down)


def last_tail(x, o, kvs, heads, w_out, gain, w_gate, w_up, w_down, layer):
    rows, model = x.shape
    _, half, inner = o.shape
    ffn = w_gate.shape[2]
    out_steps, tf = 4, TF
    slices = ffn // tf
    step = inner // out_steps
    seq, width = kvs[0].shape
    dim = width // heads
    part = seq // slices
    out_at, mlp_at, wo_spec, mlp_specs = tail_specs(layer, out_steps, slices, tf, model, step, lambda i: i)
    whole = pl.BlockSpec((rows, model), lambda i: (0, 0))
    cache = jax.ShapeDtypeStruct((layer + 1, seq * heads, dim), BF16)
    cache_spec = pl.BlockSpec((layer + 1, part * heads, dim), lambda i: (0, mlp_at(i), 0))
    return pl.pallas_call(
        functools.partial(last_kernel, out_steps, layer),
        name="tail_last",
        grid=(out_steps + slices + 1,),
        out_shape=[jax.ShapeDtypeStruct((rows, model), BF16), cache, cache],
        in_specs=[
            whole,
            pl.BlockSpec((2, half, step), lambda i: (0, 0, out_at(i))),
            wo_spec,
            pl.BlockSpec(gain.shape, lambda i: (0, 0)),
        ]
        + mlp_specs
        + [pl.BlockSpec((part, width), lambda i: (mlp_at(i), 0))] * len(kvs),
        out_specs=[whole, cache_spec, cache_spec],
        scratch_shapes=[
            pltpu.VMEM((rows, model), F32),
            pltpu.VMEM((rows, model), BF16),
            pltpu.VMEM((2, rows, tf), BF16),
            pltpu.VMEM((len(kvs), part * heads, dim), F32),
        ],
        compiler_params=pltpu.CompilerParams(vmem_limit_bytes=60 * MIB),
        cost_estimate=pl.CostEstimate(
            flops=2 * rows * model * (inner + 3 * ffn), bytes_accessed=2 * model * (inner + 3 * ffn), transcendentals=rows * ffn
        ),
    )(x, o, w_out.reshape(w_out.shape[0], inner, model), gain, w_gate, w_up, w_down, *kvs)


def solution(mesh):
    cp_size = mesh.shape["cp"]
    row_spec = P(("req", "cp"), None)
    pos_spec = P(("req", "cp"))
    rep_spec = P()
    cache_spec = P(None, "req", "cp", None)

    def per_device(hidden, positions, gain_attn, gain_mlp, w_query, w_key, w_value, w_out, w_gate, w_up, w_down):
        num_layers, model, all_heads, dim = w_query.shape
        rows = hidden.shape[0]
        cache_shape = (num_layers, cp_size * rows, all_heads // cp_size, dim)
        inv_freq = ROPE_BASE ** (-jnp.arange(0, dim, 2, dtype=F32) / dim)
        tables = [positions.reshape(rows // 128, 128), jnp.concatenate([inv_freq, inv_freq])[None]]
        kvs = []
        for layer in range(num_layers):
            o, k, v, *new = front(hidden, gain_attn, tables, w_query, w_key, w_value, cp_size, layer)
            kvs += [k, v]
            if layer == 0:
                cos_sin = new
            if layer < num_layers - 1:
                hidden, gathered = split_tail(hidden, o, cp_size, w_out, gain_mlp, gain_attn, w_gate, w_up, w_down, layer)
                tables = cos_sin + [gathered]
            else:
                hidden, k_cache, v_cache = last_tail(
                    hidden, o, kvs, all_heads // cp_size, w_out, gain_mlp, w_gate, w_up, w_down, layer
                )
        return hidden, k_cache.reshape(cache_shape), v_cache.reshape(cache_shape)

    in_specs = (row_spec, pos_spec) + (rep_spec,) * 9
    return jax.shard_map(per_device, mesh=mesh, in_specs=in_specs, out_specs=(row_spec, cache_spec, cache_spec), check_vma=False)
```

```python
import functools

import jax
import jax.numpy as jnp
from jax import lax
from jax.experimental import pallas as pl
from jax.experimental.pallas import tpu as pltpu
from jax.sharding import PartitionSpec as P

NORM_EPS = 1e-5
ROPE_BASE = 10000.0
LOG2E = 1.4426950408889634
MESH = pl.DeviceIdType.MESH
MIB = 1024 * 1024
TQ = 512
TK = 1024
SLOTS = 7
TF = 512
BF16, F32 = jnp.bfloat16, jnp.float32


def rms_norm(values, gain_vec):
    wide_vals = values.astype(F32)
    inv_rms = lax.rsqrt(jnp.mean(wide_vals * wide_vals, axis=-1, keepdims=True) + NORM_EPS)
    return (wide_vals * inv_rms * gain_vec.astype(F32)).astype(BF16)


def greet_all(n, me):
    barrier = pltpu.get_barrier_semaphore()
    for d in range(1, n):
        pl.semaphore_signal(barrier, inc=1, device_id={"cp": lax.rem(me + d, n)}, device_id_type=MESH)
    pl.semaphore_wait(barrier, n - 1)


def front_kernel(
    n, heads, dim, layer, first, more, x_ref, gain_ref, *refs
):
    if first:
        pos_ref, freq_ref, *refs = refs
    else:
        cos_in, sin_in, w_in, ha_ref, *refs = refs
    wq_ref, wk_ref, wv_ref, o_ref, k_out, v_out, *refs = refs
    if first:
        cos_out, sin_out, *refs = refs
    if more:
        w_out, w_next, *refs = refs
    if first:
        pos_buf, pos_send, pos_recv, *refs = refs
    else:
        ha_sem, *refs = refs
    h_buf, w_raw, w_buf, q_ref, k_ref, v_ref, vt_ref, cos_ref, sin_ref, o_buf, m_st, l_st, acc_st, *sems = refs
    in_sem, out_sem, w_sem, recv_sem, own_sem, fwd_sem, relay_sem, o_local, o_send, o_recv = sems
    block, model = h_buf.shape[2:]
    rows = n * block
    piece = block // 2
    width = heads * dim
    scale = LOG2E * dim**-0.5
    chips = n // 2
    me = lax.axis_index("cp")
    chip, core = me // 2, lax.rem(me, 2)

    def at(step, k):
        return 2 * lax.rem(chip + step, chips) + k

    right, left, opp, partner = at(1, core), at(chips - 1, core), at(2, core), at(0, 1 - core)
    sources = (left, right, opp)

    def remote(s, origin, p, target, sem):
        part = h_buf.at[s, origin, pl.ds(p * piece, piece)]
        return pltpu.make_async_remote_copy(
            src_ref=part, dst_ref=part, send_sem=sem, recv_sem=recv_sem.at[s, origin, p],
            device_id={"cp": target}, device_id_type=MESH,
        )

    own_sends = [(right, 0), (left, 1), (right, 1), (left, 0), (partner, 0), (partner, 1)]

    def send_own(s):
        for j, (target, p) in enumerate(own_sends):
            remote(s, me, p, target, own_sem.at[s, j]).start()

    def arrived(s, origin, p):
        remote(s, origin, p, partner, own_sem.at[s, 0]).wait_recv()

    def relay(s, j, p):
        return remote(s, sources[j], p, partner, relay_sem.at[s, j, p])

    def forward(s, way):
        return remote(s, (left, right)[way], way, (right, left)[way], fwd_sem.at[s, way])

    def pass_on(s):
        for way in range(2):
            arrived(s, (left, right)[way], way)
            forward(s, way).start()
            relay(s, way, way).start()

    def receive(s, k):
        @pl.when(k == 0)
        def _():
            for p in range(2):
                arrived(s, partner, p)

        @pl.when(k == 1)
        def _():
            for way in range(2):
                arrived(s, (left, right)[way], 1 - way)
                relay(s, way, 1 - way).start()
            for p in range(2):
                arrived(s, at(chips - 1, 1 - core), p)

        @pl.when(k == 2)
        def _():
            for p in range(2):
                arrived(s, at(1, 1 - core), p)

        @pl.when(k == 3)
        def _():
            for p in range(2):
                arrived(s, opp, p)
                relay(s, 2, p).start()
            for p in range(2):
                arrived(s, at(2, 1 - core), p)

    def ready(k):
        c = lax.rem(chip + (0, chips - 1, 1, 2)[k], chips)
        return pltpu.make_async_copy(ha_ref.at[pl.ds(2 * c, 2)], h_buf.at[0, pl.ds(2 * c, 2)], ha_sem.at[k])

    def place(s, d):
        return pl.multiple_of(jnp.where(s == 0, d * block, rows + (n - 1 - d) * block), block)

    def project(s, c):
        h = h_buf[s, pl.ds(2 * c, 2)].reshape(2 * block, model)
        key, val, query = (
            jnp.dot(h, w_buf[:, j * width : (j + 1) * width], preferred_element_type=F32) for j in (1, 2, 0)
        )
        for j in range(2):
            part = pl.ds(place(s, 2 * c + j), block)
            cos, sin = cos_ref[part, :], sin_ref[part, :]
            mine = slice(j * block, (j + 1) * block)
            for g in range(heads):
                lo, hi = g * dim, (g + 1) * dim
                for y, dst in ((key, k_ref), (query, q_ref)):
                    x = y[mine, lo:hi]
                    dst[part, lo:hi] = (x * cos + pltpu.roll(x, dim // 2, 1) * sin).astype(BF16)
            v_ref[part, :] = val[mine].astype(BF16)
            vt_ref[:, part] = val[mine].T.astype(BF16)

    def scores_of(queries, g, start, size, masked):
        k = k_ref[pl.ds(start, size), g * dim : (g + 1) * dim]
        s = lax.dot_general(k, queries[g], (((1,), (1,)), ((), ())), preferred_element_type=F32)
        if masked:
            row = lax.broadcasted_iota(jnp.int32, s.shape, 0)
            col = lax.broadcasted_iota(jnp.int32, s.shape, 1)
            s = jnp.where(row <= col, s, -jnp.inf)
        return s

    def absorb(g, s, start, size, state):
        m, l, acc = state
        m_new = jnp.maximum(m, jnp.max(s, axis=0, keepdims=True))
        a = jnp.exp2((m - m_new) * scale)
        p = jnp.exp2((s - m_new) * scale)
        l = l * a + jnp.sum(p, axis=0, keepdims=True)
        vt = vt_ref[g * dim : (g + 1) * dim, pl.ds(start, size)]
        return m_new, l, acc * a + jnp.dot(vt, p.astype(BF16), preferred_element_type=F32)

    def run(queries, parts, carry):
        carry = list(carry)
        items = [(g,) + part for part in parts for g in range(heads)]
        scores = [scores_of(queries, *item) for item in items[:2]]
        for j, (g, start, size, _) in enumerate(items):
            if j + 2 < len(items):
                scores.append(scores_of(queries, *items[j + 2]))
            carry[g] = absorb(g, scores[j], start, size, carry[g])
        return tuple(carry)

    def chunk(queries, start, size, carry, masked):
        return run(queries, [(start, size, masked)], carry)

    def chunks(queries, lo, hi, base, size, carry):
        return lax.fori_loop(
            lo, hi, lambda j, c: chunk(queries, pl.multiple_of(base + j * size, size), size, c, False), carry
        )

    def queries_at(start):
        return [q_ref[pl.ds(start, TQ), g * dim : (g + 1) * dim] for g in range(heads)]

    def fresh():
        return tuple(
            (jnp.full((1, TQ), -jnp.inf, F32), jnp.zeros((1, TQ), F32), jnp.zeros((dim, TQ), F32)) for _ in range(heads)
        )

    def finish(t, base, carry):
        start = pl.multiple_of(base + t * TQ, TQ)
        queries = queries_at(start)
        per = TK // TQ
        full = t // per
        carry = chunks(queries, 0, full, base, TK, carry)
        carry = chunks(queries, full * per, t, base, TQ, carry)
        carry = chunk(queries, start, TQ, carry, True)
        for g in range(heads):
            m, l, acc = carry[g]
            o_buf[pl.ds(start, TQ), g * dim : (g + 1) * dim] = (acc / l).T.astype(BF16)

    outs = (o_ref.at[0], o_ref.at[1])
    gathers = (0, 1) if first else (1,)

    def own_result(s):
        cols = pl.ds(pl.multiple_of(me * width, width), width)
        return pltpu.make_async_copy(o_buf.at[pl.ds(place(s, me), block), :], outs[s].at[:, cols], o_local.at[s])

    def result(s, d, source):
        cols = pl.ds(pl.multiple_of(source * width, width), width)
        return pltpu.make_async_remote_copy(
            src_ref=o_buf.at[pl.ds(place(s, d), block), :], dst_ref=outs[s].at[:, cols],
            send_sem=o_send.at[s, d], recv_sem=o_recv.at[s, source],
            device_id={"cp": d}, device_id_type=MESH,
        )

    def weights(of, j):
        return pltpu.make_async_copy((wq_ref, wk_ref, wv_ref)[j].at[of, :, me], w_raw.at[j], w_sem.at[j])

    def unpack(dst):
        per = model // 256

        def step(i, _):
            j, part = i // per, pl.ds(pl.multiple_of(lax.rem(i, per) * 256, 256), 256)
            w = w_raw[j, part]
            for g in range(heads):
                dst[part, pl.ds(pl.multiple_of(j * width + g * dim, dim), dim)] = w[:, g, :]
            return 0

        lax.fori_loop(0, 3 * per, step, 0)

    if first:
        loads = [weights(layer, j) for j in range(3)]
    else:
        loads = [
            pltpu.make_async_copy(src, dst, in_sem.at[j])
            for j, (src, dst) in enumerate(((cos_in, cos_ref), (sin_in, sin_ref), (w_in, w_buf)))
        ] + ([weights(layer + 1, j) for j in range(3)] if more else [])
    for load in loads:
        load.start()
    if not first:
        for k in range(chips):
            ready(k).start()
    for s in gathers:
        h_buf[s, me] = rms_norm(x_ref[s * block : (s + 1) * block, :], gain_ref[layer : layer + 1, :])
    greet_all(n, me)
    if first:
        def pos_copy(d, slot):
            return pltpu.make_async_remote_copy(
                src_ref=pos_ref, dst_ref=pos_buf.at[slot], send_sem=pos_send.at[d], recv_sem=pos_recv.at[slot],
                device_id={"cp": lax.rem(me + d, n)}, device_id_type=MESH,
            )

        for d in range(1, n):
            pos_copy(d, me).start()
    send_own(gathers[0])
    if first:
        pos_buf[me] = pos_ref[...]
    for j in range(3):
        loads[j].wait()
    if first:
        unpack(w_buf)
        if more:
            for j in range(3):
                weights(layer + 1, j).start()
        pass_on(0)
        send_own(1)
    if more:
        for j in range(3):
            weights(layer + 1, j).wait()
        unpack(w_next)
        for d in range(1, n):
            pos_copy(d, me).wait_send()
            pos_copy(d, lax.rem(me + d, n)).wait_recv()
        sign = jnp.where(lax.broadcasted_iota(jnp.int32, (1, dim), 1) < dim // 2, -1.0, 1.0).astype(F32)

        def tables(s, c):
            per = block // 128

            def step(i, _):
                d, j = 2 * c + i // per, lax.rem(i, per)
                pos = pos_buf[d, pl.ds(s * per + j, 1), :].astype(F32)
                angles = jnp.broadcast_to(pos, (128, 128)).T * freq_ref[...]
                part = pl.ds(pl.multiple_of(place(s, d) + j * 128, 128), 128)
                cos_ref[part, :] = jnp.cos(angles)
                sin_ref[part, :] = jnp.sin(angles) * sign
                return 0

            lax.fori_loop(0, 2 * per, step, 0)

    saves = [(k_ref, k_out), (v_ref, v_out)]
    if first:
        saves += [(cos_ref, cos_out), (sin_ref, sin_out)]
    if more:
        saves.append((w_next, w_out))

    def save(j):
        return pltpu.make_async_copy(*saves[j], out_sem.at[j])

    def half(s, _):
        @pl.when(s == 1)
        def _():
            if first:
                pass_on(1)
            own_result(0).start()
            for d in range(1, n):
                result(0, lax.rem(me + d, n), me).start()

        def step(k, _):
            c = lax.rem(chip + jnp.where(k == 0, 0, jnp.where(k == 1, chips - 1, k - 1)), chips)
            if first:
                tables(s, c)
                receive(s, k)
            else:
                for j in range(chips):

                    @pl.when((s == 0) & (k == j))
                    def _(j=j):
                        ready(j).wait()

                @pl.when(s == 1)
                def _():
                    receive(1, k)

            project(s, c)

            def put(t, carry):
                for g in range(heads):
                    m_st[t, g], l_st[t, g], acc_st[t, g] = carry[g]

            @pl.when(s == 0)
            def _():
                put(c, fresh())

            @pl.when(s == 1)
            def _():
                t = chips - 1 - c
                queries = queries_at(pl.multiple_of(rows + t * TQ, TQ))
                put(t, run(queries, [(j * TK, TK, False) for j in range(rows // TK)], fresh()))

            return 0

        lax.fori_loop(0, chips, step, 0)
        if not first:

            @pl.when(s == 0)
            def _():
                pass_on(1)

        @pl.when(s == 1)
        def _():
            for j in range(len(saves)):
                save(j).start()

        def tile(i, _):
            t = lax.rem(i + chip, chips)
            finish(t, s * rows, tuple((m_st[t, g], l_st[t, g], acc_st[t, g]) for g in range(heads)))

            @pl.when(s == 1)
            def _():
                for j in range(2):
                    d = n - 1 - (2 * t + j)

                    @pl.when(d == me)
                    def _():
                        own_result(1).start()

                    @pl.when(d != me)
                    def _():
                        result(1, d, me).start()

            return 0

        lax.fori_loop(0, chips, tile, 0)
        return 0

    lax.fori_loop(0, 2, half, 0)
    for j in range(len(saves)):
        save(j).wait()
    for s in gathers:
        for j, (target, p) in enumerate(own_sends):
            remote(s, me, p, target, own_sem.at[s, j]).wait_send()
        for way in range(2):
            forward(s, way).wait_send()
        for j in range(3):
            for p in range(2):
                relay(s, j, p).wait_send()
    for s in range(2):
        own_result(s).wait()
        for d in range(1, n):
            other = lax.rem(me + d, n)
            result(s, other, me).wait_send()
            result(s, other, other).wait_recv()


def front(x, gain, tables, w_query, w_key, w_value, n, layer):
    first = layer == 0
    rows, model = x.shape
    num_layers, _, all_heads, dim = w_query.shape
    more = layer < num_layers - 1
    heads = all_heads // n
    width = heads * dim
    block = rows // 2
    seq = n * rows
    vmem = pl.BlockSpec(memory_space=pltpu.VMEM)
    hbm = pl.BlockSpec(memory_space=pl.ANY)
    chips = n // 2
    out = jax.ShapeDtypeStruct((2, block, all_heads * dim), BF16)
    kv = jax.ShapeDtypeStruct((seq, width), BF16)
    table = jax.ShapeDtypeStruct((seq, dim), F32)
    packed = jax.ShapeDtypeStruct((model, 3 * width), BF16)
    dma = pltpu.SemaphoreType.DMA
    pos_scratch = [pltpu.VMEM((n,) + tables[0].shape, jnp.int32), dma((n,)), dma((n,))] if first else [dma((chips,))]
    by_head = [w.reshape(num_layers, model, n, heads, dim) for w in (w_query, w_key, w_value)]
    return pl.pallas_call(
        functools.partial(front_kernel, n, heads, dim, layer, first, more),
        name="front",
        out_shape=[out, kv, kv] + [table, table] * first + [packed] * more,
        in_specs=[vmem] * (4 if first else 2) + [hbm] * (3 if first else 7),
        out_specs=[hbm] * (3 + 2 * first + more),
        scratch_shapes=[pltpu.VMEM(packed.shape, BF16)] * more
        + pos_scratch
        + [
            pltpu.VMEM((2, n, block, model), BF16),
            pltpu.VMEM((3, model, heads, dim), BF16),
            pltpu.VMEM((model, 3 * width), BF16),
            pltpu.VMEM((seq, width), BF16),
            pltpu.VMEM((seq, width), BF16),
            pltpu.VMEM((seq, width), BF16),
            pltpu.VMEM((width, seq), BF16),
            pltpu.VMEM((seq, dim), F32),
            pltpu.VMEM((seq, dim), F32),
            pltpu.VMEM((seq, width), BF16),
            pltpu.VMEM((chips, heads, 1, TQ), F32),
            pltpu.VMEM((chips, heads, 1, TQ), F32),
            pltpu.VMEM((chips, heads, dim, TQ), F32),
            dma((3,)),
            dma((5,)),
            dma((3,)),
            dma((2, n, 2)),
            dma((2, 6)),
            dma((2, 2)),
            dma((2, 3, 2)),
            dma((2,)),
            dma((2, n)),
            dma((2, n)),
        ],
        compiler_params=pltpu.CompilerParams(vmem_limit_bytes=62 * MIB, collective_id=layer + 1, has_side_effects=True),
        cost_estimate=pl.CostEstimate(flops=6 * seq * model * width + 2 * seq * seq * width, bytes_accessed=seq * model * 2, transcendentals=seq * seq * heads // 2),
    )(x, gain, *tables, *by_head)


def mlp_parts(acc, normed, act, wg_ref, wu_ref, wd_ref, now):
    def gate_up(slot=0):
        h = normed[...]
        gate = jnp.dot(h, wg_ref[slot], preferred_element_type=F32)
        up = jnp.dot(h, wu_ref[slot], preferred_element_type=F32)
        act[now] = (jax.nn.silu(gate) * up).astype(BF16)

    def down(slot=0):
        acc[...] += jnp.dot(act[1 - now], wd_ref[slot], preferred_element_type=F32)

    return gate_up, down


def out_step(r, out_steps, layer, x_ref, o_ref, wo_ref, gain_ref, acc, normed):
    o = o_ref[...].reshape(acc.shape[0], o_ref.shape[2])
    part = jnp.dot(o, wo_ref[0], preferred_element_type=F32)

    @pl.when(r == 0)
    def _():
        acc[...] = part

    @pl.when(r > 0)
    def _():
        acc[...] += part

    @pl.when(r == out_steps - 1)
    def _():
        x = (x_ref[...].astype(F32) + acc[...]).astype(BF16)
        normed[...] = rms_norm(x, gain_ref[layer : layer + 1, :])
        acc[...] = x.astype(F32)


def last_kernel(
    out_steps, layer, x_ref, o_ref, wo_ref, gain_ref, wg_ref, wu_ref, wd_ref, *refs
):
    kv_refs = refs[: 2 * (layer + 1)]
    y_ref, kc_ref, vc_ref, acc, normed, act, mixed = refs[2 * (layer + 1) :]
    i = pl.program_id(0)
    last = pl.num_programs(0) - 1
    gate_up, down = mlp_parts(acc, normed, act, wg_ref, wu_ref, wd_ref, lax.rem(i, 2))

    @pl.when(i < out_steps)
    def _():
        out_step(i, out_steps, layer, x_ref, o_ref, wo_ref, gain_ref, acc, normed)

    def caches():
        dim = kc_ref.shape[2]
        for j, src in enumerate(kv_refs):
            count, heads = src.shape[0], src.shape[1] // dim
            for g in range(heads):
                mixed[j, pl.ds(g, count, stride=heads), :] = src[:, g * dim : (g + 1) * dim].astype(F32)
            (kc_ref, vc_ref)[j % 2][j // 2] = mixed[j].astype(BF16)

    @pl.when(i == out_steps)
    def _():
        gate_up()
        caches()

    @pl.when((i > out_steps) & (i < last))
    def _():
        down()
        gate_up()
        caches()

    @pl.when(i == last)
    def _():
        down()
        y_ref[...] = acc[...].astype(BF16)


def split_kernel(
    n, out_steps, layer, steps, x_ref, o_ref, wo_ref, gain_ref, next_gain_ref, wg_ref, wu_ref, wd_ref,
    y_ref, ha_ref, acc, normed, act, mine, wg_buf, wu_buf, wd_buf, w_sem, local_sem, recv_sem, own_sem, fwd_sem, relay_sem,
):
    i = pl.program_id(0)
    s, r = i // steps, lax.rem(i, steps)
    gate_up, down = mlp_parts(acc, normed, act, wg_buf, wu_buf, wd_buf, lax.rem(i, 2))
    slots, tf = wd_buf.shape[:2]
    slices = steps - out_steps - 1

    def load(kind, f):
        cols = pl.ds(pl.multiple_of(f * tf, tf), tf)
        src = (wg_ref.at[layer, :, cols], wu_ref.at[layer, :, cols], wd_ref.at[layer, cols])[kind]
        slot = lax.rem(f, slots)
        return pltpu.make_async_copy(src, (wg_buf, wu_buf, wd_buf)[kind].at[slot], w_sem.at[kind, slot])

    def slice_at(j):
        return jnp.where(s == 0, j, slices - 1 - j)

    def await_loads(kinds, f):
        @pl.when((s == 0) | (f < slices - slots))
        def _():
            for kind in kinds:
                load(kind, f).wait()

    def refill(kinds, f):
        after = jnp.where(s == 0, f + slots, f - slots)

        @pl.when((after >= 0) & (after < slices))
        def _():
            for kind in kinds:
                load(kind, after).start()

    f_up = slice_at(r - out_steps)
    f_down = slice_at(r - out_steps - 1)

    @pl.when(i == 0)
    def _():
        for f in range(slots):
            for kind in range(3):
                load(kind, f).start()
    piece = mine.shape[0] // 2
    chips = n // 2
    me = lax.axis_index("cp")
    chip, core = me // 2, lax.rem(me, 2)

    def at(step, k):
        return 2 * lax.rem(chip + step, chips) + k

    right, left, opp, partner = at(1, core), at(chips - 1, core), at(2, core), at(0, 1 - core)
    sources = (left, right, opp)
    own_sends = [(right, 0), (left, 1), (right, 1), (left, 0), (partner, 0), (partner, 1)]
    barrier = pltpu.get_barrier_semaphore()

    def remote(src, origin, p, target, sem):
        return pltpu.make_async_remote_copy(
            src_ref=src, dst_ref=ha_ref.at[origin, pl.ds(p * piece, piece)], send_sem=sem,
            recv_sem=recv_sem.at[origin, p], device_id={"cp": target}, device_id_type=MESH,
        )

    def held(origin, p):
        return ha_ref.at[origin, pl.ds(p * piece, piece)]

    def own(j):
        target, p = own_sends[j]
        return remote(mine.at[pl.ds(p * piece, piece)], me, p, target, own_sem.at[j])

    def keep():
        return pltpu.make_async_copy(mine, ha_ref.at[me], local_sem)

    def arrived(origin, p):
        remote(held(origin, p), origin, p, partner, own_sem.at[0]).wait_recv()

    def relay(j, p):
        return remote(held(sources[j], p), sources[j], p, partner, relay_sem.at[j, p])

    def forward(way):
        origin = (left, right)[way]
        return remote(held(origin, way), origin, way, (right, left)[way], fwd_sem.at[way])

    @pl.when(i == 0)
    def _():
        for d in range(1, n):
            pl.semaphore_signal(barrier, inc=1, device_id={"cp": lax.rem(me + d, n)}, device_id_type=MESH)
        pl.semaphore_wait(barrier, n - 1)

    @pl.when(i == steps + out_steps + 5)
    def _():
        for way in range(2):
            arrived((left, right)[way], way)
            forward(way).start()
            relay(way, way).start()

    @pl.when(i == steps + out_steps + 11)
    def _():
        for way in range(2):
            arrived((left, right)[way], 1 - way)
            relay(way, 1 - way).start()

    @pl.when(i == 2 * steps - 1)
    def _():
        for p in range(2):
            arrived(opp, p)
            relay(2, p).start()

    @pl.when(r < out_steps)
    def _():
        out_step(r, out_steps, layer, x_ref, o_ref, wo_ref, gain_ref, acc, normed)

    @pl.when((r >= out_steps) & (r < steps - 1))
    def _():
        await_loads((0, 1), f_up)

    @pl.when(r > out_steps)
    def _():
        await_loads((2,), f_down)

    @pl.when(r == out_steps)
    def _():
        gate_up(lax.rem(f_up, slots))

    @pl.when((r > out_steps) & (r < steps - 1))
    def _():
        down(lax.rem(f_down, slots))
        gate_up(lax.rem(f_up, slots))

    @pl.when(r == steps - 1)
    def _():
        down(lax.rem(f_down, slots))
        y_ref[...] = acc[...].astype(BF16)

    @pl.when((r >= out_steps) & (r < steps - 1))
    def _():
        refill((0, 1), f_up)

    @pl.when(r > out_steps)
    def _():
        refill((2,), f_down)

    @pl.when(i == steps - 1)
    def _():
        mine[...] = rms_norm(y_ref[...], next_gain_ref[layer + 1 : layer + 2, :])
        keep().start()
        for j in range(len(own_sends)):
            own(j).start()

    @pl.when(i == 2 * steps - 1)
    def _():
        keep().wait()
        for j in range(len(own_sends)):
            own(j).wait_send()
        for way in range(2):
            forward(way).wait_send()
        for j in range(3):
            for p in range(2):
                relay(j, p).wait_send()
        for origin in (partner, at(chips - 1, 1 - core), at(1, 1 - core), at(2, 1 - core)):
            for p in range(2):
                arrived(origin, p)


def tail_specs(layer, out_steps, slices, tf, model, step, r_of):
    out_at = lambda i: jnp.minimum(r_of(i), out_steps - 1)
    mlp_at = lambda i: jnp.clip(r_of(i) - out_steps, 0, slices - 1)
    down_at = lambda i: jnp.clip(r_of(i) - out_steps - 1, 0, slices - 1)
    w_out = pl.BlockSpec((1, step, model), lambda i: (layer, out_at(i), 0))
    mlp = [
        pl.BlockSpec((1, model, tf), lambda i: (layer, 0, mlp_at(i))),
        pl.BlockSpec((1, model, tf), lambda i: (layer, 0, mlp_at(i))),
        pl.BlockSpec((1, tf, model), lambda i: (layer, down_at(i), 0)),
    ]
    return out_at, mlp_at, w_out, mlp


def split_tail(x, o, n, w_out, gain, next_gain, w_gate, w_up, w_down, layer):
    rows, model = x.shape
    _, half, inner = o.shape
    ffn = w_gate.shape[2]
    out_steps, tf, slots = 2, TF, SLOTS
    slices = ffn // tf
    step = inner // out_steps
    steps = out_steps + slices + 1
    out_at, _, wo_spec, _ = tail_specs(layer, out_steps, slices, tf, model, step, lambda i: lax.rem(i, steps))
    hbm = pl.BlockSpec(memory_space=pl.ANY)
    part = pl.BlockSpec((half, model), lambda i: (i // steps, 0))
    full = pl.BlockSpec(gain.shape, lambda i: (0, 0))
    dma = pltpu.SemaphoreType.DMA
    return pl.pallas_call(
        functools.partial(split_kernel, n, out_steps, layer, steps),
        name="tail_split",
        grid=(2 * steps,),
        out_shape=[jax.ShapeDtypeStruct((rows, model), BF16), jax.ShapeDtypeStruct((n, half, model), BF16)],
        in_specs=[part, pl.BlockSpec((1, half, step), lambda i: (i // steps, 0, out_at(i))), wo_spec, full, full, hbm, hbm, hbm],
        out_specs=[part, pl.BlockSpec(memory_space=pl.ANY)],
        scratch_shapes=[
            pltpu.VMEM((half, model), F32),
            pltpu.VMEM((half, model), BF16),
            pltpu.VMEM((2, half, tf), BF16),
            pltpu.VMEM((half, model), BF16),
            pltpu.VMEM((slots, model, tf), BF16),
            pltpu.VMEM((slots, model, tf), BF16),
            pltpu.VMEM((slots, tf, model), BF16),
            dma((3, slots)),
            dma,
            dma((n, 2)),
            dma((6,)),
            dma((2,)),
            dma((3, 2)),
        ],
        compiler_params=pltpu.CompilerParams(vmem_limit_bytes=63 * MIB, collective_id=8 + layer, has_side_effects=True),
        cost_estimate=pl.CostEstimate(
            flops=2 * rows * model * (inner + 3 * ffn), bytes_accessed=4 * model * (inner + 3 * ffn), transcendentals=rows * ffn
        ),
    )(x, o, w_out.reshape(w_out.shape[0], inner, model), gain, next_gain, w_gate, w_up, w_down)


def last_tail(x, o, kvs, heads, w_out, gain, w_gate, w_up, w_down, layer):
    rows, model = x.shape
    _, half, inner = o.shape
    ffn = w_gate.shape[2]
    out_steps, tf = 4, TF
    slices = ffn // tf
    step = inner // out_steps
    seq, width = kvs[0].shape
    dim = width // heads
    part = seq // slices
    out_at, mlp_at, wo_spec, mlp_specs = tail_specs(layer, out_steps, slices, tf, model, step, lambda i: i)
    whole = pl.BlockSpec((rows, model), lambda i: (0, 0))
    cache = jax.ShapeDtypeStruct((layer + 1, seq * heads, dim), BF16)
    cache_spec = pl.BlockSpec((layer + 1, part * heads, dim), lambda i: (0, mlp_at(i), 0))
    return pl.pallas_call(
        functools.partial(last_kernel, out_steps, layer),
        name="tail_last",
        grid=(out_steps + slices + 1,),
        out_shape=[jax.ShapeDtypeStruct((rows, model), BF16), cache, cache],
        in_specs=[
            whole,
            pl.BlockSpec((2, half, step), lambda i: (0, 0, out_at(i))),
            wo_spec,
            pl.BlockSpec(gain.shape, lambda i: (0, 0)),
        ]
        + mlp_specs
        + [pl.BlockSpec((part, width), lambda i: (mlp_at(i), 0))] * len(kvs),
        out_specs=[whole, cache_spec, cache_spec],
        scratch_shapes=[
            pltpu.VMEM((rows, model), F32),
            pltpu.VMEM((rows, model), BF16),
            pltpu.VMEM((2, rows, tf), BF16),
            pltpu.VMEM((len(kvs), part * heads, dim), F32),
        ],
        compiler_params=pltpu.CompilerParams(vmem_limit_bytes=60 * MIB),
        cost_estimate=pl.CostEstimate(
            flops=2 * rows * model * (inner + 3 * ffn), bytes_accessed=2 * model * (inner + 3 * ffn), transcendentals=rows * ffn
        ),
    )(x, o, w_out.reshape(w_out.shape[0], inner, model), gain, w_gate, w_up, w_down, *kvs)


def solution(mesh):
    cp_size = mesh.shape["cp"]
    row_spec = P(("req", "cp"), None)
    pos_spec = P(("req", "cp"))
    rep_spec = P()
    cache_spec = P(None, "req", "cp", None)

    def per_device(hidden, positions, gain_attn, gain_mlp, w_query, w_key, w_value, w_out, w_gate, w_up, w_down):
        num_layers, model, all_heads, dim = w_query.shape
        rows = hidden.shape[0]
        cache_shape = (num_layers, cp_size * rows, all_heads // cp_size, dim)
        inv_freq = ROPE_BASE ** (-jnp.arange(0, dim, 2, dtype=F32) / dim)
        tables = [positions.reshape(rows // 128, 128), jnp.concatenate([inv_freq, inv_freq])[None]]
        kvs = []
        for layer in range(num_layers):
            o, k, v, *new = front(hidden, gain_attn, tables, w_query, w_key, w_value, cp_size, layer)
            kvs += [k, v]
            if layer == 0:
                cos_sin, new = new[:2], new[2:]
            if layer < num_layers - 1:
                hidden, gathered = split_tail(hidden, o, cp_size, w_out, gain_mlp, gain_attn, w_gate, w_up, w_down, layer)
                tables = cos_sin + new + [gathered]
            else:
                hidden, k_cache, v_cache = last_tail(
                    hidden, o, kvs, all_heads // cp_size, w_out, gain_mlp, w_gate, w_up, w_down, layer
                )
        return hidden, k_cache.reshape(cache_shape), v_cache.reshape(cache_shape)

    in_specs = (row_spec, pos_spec) + (rep_spec,) * 9
    return jax.shard_map(per_device, mesh=mesh, in_specs=in_specs, out_specs=(row_spec, cache_spec, cache_spec), check_vma=False)
```

```python
import functools

import jax
import jax.numpy as jnp
from jax import lax
from jax.experimental import pallas as pl
from jax.experimental.pallas import tpu as pltpu
from jax.sharding import PartitionSpec as P

NORM_EPS = 1e-5
ROPE_BASE = 10000.0
LOG2E = 1.4426950408889634
MESH = pl.DeviceIdType.MESH
MIB = 1024 * 1024
TQ = 512
TK = 1024
SLOTS = 7
TF = 512
BF16, F32 = jnp.bfloat16, jnp.float32


def rms_norm(values, gain_vec):
    wide_vals = values.astype(F32)
    inv_rms = lax.rsqrt(jnp.mean(wide_vals * wide_vals, axis=-1, keepdims=True) + NORM_EPS)
    return (wide_vals * inv_rms * gain_vec.astype(F32)).astype(BF16)


def greet_all(n, me):
    barrier = pltpu.get_barrier_semaphore()
    for d in range(1, n):
        pl.semaphore_signal(barrier, inc=1, device_id={"cp": lax.rem(me + d, n)}, device_id_type=MESH)
    pl.semaphore_wait(barrier, n - 1)


def front_kernel(
    n, heads, dim, layer, first, more, x_ref, gain_ref, *refs
):
    if first:
        pos_ref, freq_ref, *refs = refs
    else:
        cos_in, sin_in, w_in, ha_ref, *refs = refs
    wq_ref, wk_ref, wv_ref, o_ref, k_out, v_out, *refs = refs
    if first:
        cos_out, sin_out, *refs = refs
    if more:
        w_out, w_next, *refs = refs
    if first:
        pos_buf, pos_send, pos_recv, *refs = refs
    else:
        ha_sem, *refs = refs
    h_buf, w_raw, w_buf, q_ref, k_ref, v_ref, vt_ref, cos_ref, sin_ref, o_buf, m_st, l_st, acc_st, *sems = refs
    in_sem, out_sem, w_sem, recv_sem, own_sem, fwd_sem, relay_sem, o_local, o_send, o_recv = sems
    block, model = h_buf.shape[2:]
    rows = n * block
    piece = block // 2
    width = heads * dim
    scale = LOG2E * dim**-0.5
    chips = n // 2
    me = lax.axis_index("cp")
    chip, core = me // 2, lax.rem(me, 2)

    def at(step, k):
        return 2 * lax.rem(chip + step, chips) + k

    right, left, opp, partner = at(1, core), at(chips - 1, core), at(2, core), at(0, 1 - core)
    sources = (left, right, opp)

    def remote(s, origin, p, target, sem):
        part = h_buf.at[s, origin, pl.ds(p * piece, piece)]
        return pltpu.make_async_remote_copy(
            src_ref=part, dst_ref=part, send_sem=sem, recv_sem=recv_sem.at[s, origin, p],
            device_id={"cp": target}, device_id_type=MESH,
        )

    own_sends = [(right, 0), (left, 1), (right, 1), (left, 0), (partner, 0), (partner, 1)]

    def send_own(s):
        for j, (target, p) in enumerate(own_sends):
            remote(s, me, p, target, own_sem.at[s, j]).start()

    def arrived(s, origin, p):
        remote(s, origin, p, partner, own_sem.at[s, 0]).wait_recv()

    def relay(s, j, p):
        return remote(s, sources[j], p, partner, relay_sem.at[s, j, p])

    def forward(s, way):
        return remote(s, (left, right)[way], way, (right, left)[way], fwd_sem.at[s, way])

    def pass_on(s):
        for way in range(2):
            arrived(s, (left, right)[way], way)
            forward(s, way).start()
            relay(s, way, way).start()

    def receive(s, k):
        @pl.when(k == 0)
        def _():
            for p in range(2):
                arrived(s, partner, p)

        @pl.when(k == 1)
        def _():
            for way in range(2):
                arrived(s, (left, right)[way], 1 - way)
                relay(s, way, 1 - way).start()
            for p in range(2):
                arrived(s, at(chips - 1, 1 - core), p)

        @pl.when(k == 2)
        def _():
            for p in range(2):
                arrived(s, at(1, 1 - core), p)

        @pl.when(k == 3)
        def _():
            for p in range(2):
                arrived(s, opp, p)
                relay(s, 2, p).start()
            for p in range(2):
                arrived(s, at(2, 1 - core), p)

    def ready(k):
        c = lax.rem(chip + (0, chips - 1, 1, 2)[k], chips)
        return pltpu.make_async_copy(ha_ref.at[pl.ds(2 * c, 2)], h_buf.at[0, pl.ds(2 * c, 2)], ha_sem.at[k])

    def place(s, d):
        return pl.multiple_of(jnp.where(s == 0, d * block, rows + (n - 1 - d) * block), block)

    def project(s, c):
        h = h_buf[s, pl.ds(2 * c, 2)].reshape(2 * block, model)
        key, val, query = (
            jnp.dot(h, w_buf[:, j * width : (j + 1) * width], preferred_element_type=F32) for j in (1, 2, 0)
        )
        for j in range(2):
            part = pl.ds(place(s, 2 * c + j), block)
            cos, sin = cos_ref[part, :], sin_ref[part, :]
            mine = slice(j * block, (j + 1) * block)
            for g in range(heads):
                lo, hi = g * dim, (g + 1) * dim
                for y, dst in ((key, k_ref), (query, q_ref)):
                    x = y[mine, lo:hi]
                    dst[part, lo:hi] = (x * cos + pltpu.roll(x, dim // 2, 1) * sin).astype(BF16)
            v_ref[part, :] = val[mine].astype(BF16)
            vt_ref[:, part] = val[mine].T.astype(BF16)

    def scores_of(queries, g, start, size, masked):
        k = k_ref[pl.ds(start, size), g * dim : (g + 1) * dim]
        s = lax.dot_general(k, queries[g], (((1,), (1,)), ((), ())), preferred_element_type=F32)
        if masked:
            row = lax.broadcasted_iota(jnp.int32, s.shape, 0)
            col = lax.broadcasted_iota(jnp.int32, s.shape, 1)
            s = jnp.where(row <= col, s, -jnp.inf)
        return s

    def absorb(g, s, start, size, state):
        m, l, acc = state
        m_new = jnp.maximum(m, jnp.max(s, axis=0, keepdims=True))
        a = jnp.exp2((m - m_new) * scale)
        p = jnp.exp2((s - m_new) * scale)
        l = l * a + jnp.sum(p, axis=0, keepdims=True)
        vt = vt_ref[g * dim : (g + 1) * dim, pl.ds(start, size)]
        return m_new, l, acc * a + jnp.dot(vt, p.astype(BF16), preferred_element_type=F32)

    def run(queries, parts, carry):
        carry = list(carry)
        items = [(g,) + part for part in parts for g in range(heads)]
        scores = [scores_of(queries, *item) for item in items[:2]]
        for j, (g, start, size, _) in enumerate(items):
            if j + 2 < len(items):
                scores.append(scores_of(queries, *items[j + 2]))
            carry[g] = absorb(g, scores[j], start, size, carry[g])
        return tuple(carry)

    def chunk(queries, start, size, carry, masked):
        return run(queries, [(start, size, masked)], carry)

    def chunks(queries, lo, hi, base, size, carry):
        return lax.fori_loop(
            lo, hi, lambda j, c: chunk(queries, pl.multiple_of(base + j * size, size), size, c, False), carry
        )

    def queries_at(start):
        return [q_ref[pl.ds(start, TQ), g * dim : (g + 1) * dim] for g in range(heads)]

    def fresh():
        return tuple(
            (jnp.full((1, TQ), -jnp.inf, F32), jnp.zeros((1, TQ), F32), jnp.zeros((dim, TQ), F32)) for _ in range(heads)
        )

    def finish(t, base, carry):
        start = pl.multiple_of(base + t * TQ, TQ)
        queries = queries_at(start)
        per = TK // TQ
        full = t // per
        carry = chunks(queries, 0, full, base, TK, carry)
        carry = lax.cond(
            t > full * per,
            lambda c: run(queries, [(pl.multiple_of(start - TQ, TQ), TQ, False), (start, TQ, True)], c),
            lambda c: run(queries, [(start, TQ, True)], c),
            carry,
        )
        for g in range(heads):
            m, l, acc = carry[g]
            o_buf[pl.ds(start, TQ), g * dim : (g + 1) * dim] = (acc / l).T.astype(BF16)

    outs = (o_ref.at[0], o_ref.at[1])
    gathers = (0, 1) if first else (1,)

    def own_result(s):
        cols = pl.ds(pl.multiple_of(me * width, width), width)
        return pltpu.make_async_copy(o_buf.at[pl.ds(place(s, me), block), :], outs[s].at[:, cols], o_local.at[s])

    def result(s, d, source):
        cols = pl.ds(pl.multiple_of(source * width, width), width)
        return pltpu.make_async_remote_copy(
            src_ref=o_buf.at[pl.ds(place(s, d), block), :], dst_ref=outs[s].at[:, cols],
            send_sem=o_send.at[s, d], recv_sem=o_recv.at[s, source],
            device_id={"cp": d}, device_id_type=MESH,
        )

    def weights(of, j):
        return pltpu.make_async_copy((wq_ref, wk_ref, wv_ref)[j].at[of, :, me], w_raw.at[j], w_sem.at[j])

    def unpack(dst):
        per = model // 256

        def step(i, _):
            j, part = i // per, pl.ds(pl.multiple_of(lax.rem(i, per) * 256, 256), 256)
            w = w_raw[j, part]
            for g in range(heads):
                dst[part, pl.ds(pl.multiple_of(j * width + g * dim, dim), dim)] = w[:, g, :]
            return 0

        lax.fori_loop(0, 3 * per, step, 0)

    if first:
        loads = [weights(layer, j) for j in range(3)]
    else:
        loads = [
            pltpu.make_async_copy(src, dst, in_sem.at[j])
            for j, (src, dst) in enumerate(((cos_in, cos_ref), (sin_in, sin_ref), (w_in, w_buf)))
        ] + ([weights(layer + 1, j) for j in range(3)] if more else [])
    for load in loads:
        load.start()
    if not first:
        for k in range(chips):
            ready(k).start()
    for s in gathers:
        h_buf[s, me] = rms_norm(x_ref[s * block : (s + 1) * block, :], gain_ref[layer : layer + 1, :])
    greet_all(n, me)
    if first:
        def pos_copy(d, slot):
            return pltpu.make_async_remote_copy(
                src_ref=pos_ref, dst_ref=pos_buf.at[slot], send_sem=pos_send.at[d], recv_sem=pos_recv.at[slot],
                device_id={"cp": lax.rem(me + d, n)}, device_id_type=MESH,
            )

        for d in range(1, n):
            pos_copy(d, me).start()
    send_own(gathers[0])
    if first:
        pos_buf[me] = pos_ref[...]
    for j in range(3):
        loads[j].wait()
    if first:
        unpack(w_buf)
        if more:
            for j in range(3):
                weights(layer + 1, j).start()
        pass_on(0)
        send_own(1)
    if more:
        for j in range(3):
            weights(layer + 1, j).wait()
        unpack(w_next)
        for d in range(1, n):
            pos_copy(d, me).wait_send()
            pos_copy(d, lax.rem(me + d, n)).wait_recv()
        sign = jnp.where(lax.broadcasted_iota(jnp.int32, (1, dim), 1) < dim // 2, -1.0, 1.0).astype(F32)

        def tables(s, c):
            per = block // 128

            def step(i, _):
                d, j = 2 * c + i // per, lax.rem(i, per)
                pos = pos_buf[d, pl.ds(s * per + j, 1), :].astype(F32)
                angles = jnp.broadcast_to(pos, (128, 128)).T * freq_ref[...]
                part = pl.ds(pl.multiple_of(place(s, d) + j * 128, 128), 128)
                cos_ref[part, :] = jnp.cos(angles)
                sin_ref[part, :] = jnp.sin(angles) * sign
                return 0

            lax.fori_loop(0, 2 * per, step, 0)

    saves = [(k_ref, k_out), (v_ref, v_out)]
    if first:
        saves += [(cos_ref, cos_out), (sin_ref, sin_out)]
    if more:
        saves.append((w_next, w_out))

    def save(j):
        return pltpu.make_async_copy(*saves[j], out_sem.at[j])

    def half(s, _):
        @pl.when(s == 1)
        def _():
            if first:
                pass_on(1)
            own_result(0).start()
            for d in range(1, n):
                result(0, lax.rem(me + d, n), me).start()

        def step(k, _):
            c = lax.rem(chip + jnp.where(k == 0, 0, jnp.where(k == 1, chips - 1, k - 1)), chips)
            if first:
                tables(s, c)
                receive(s, k)
            else:
                for j in range(chips):

                    @pl.when((s == 0) & (k == j))
                    def _(j=j):
                        ready(j).wait()

                @pl.when(s == 1)
                def _():
                    receive(1, k)

            project(s, c)

            def put(t, carry):
                for g in range(heads):
                    m_st[t, g], l_st[t, g], acc_st[t, g] = carry[g]

            @pl.when(s == 0)
            def _():
                put(c, fresh())

            @pl.when(s == 1)
            def _():
                t = chips - 1 - c
                queries = queries_at(pl.multiple_of(rows + t * TQ, TQ))
                put(t, run(queries, [(j * TK, TK, False) for j in range(rows // TK)], fresh()))

            return 0

        lax.fori_loop(0, chips, step, 0)
        if not first:

            @pl.when(s == 0)
            def _():
                pass_on(1)

        @pl.when(s == 1)
        def _():
            for j in range(len(saves)):
                save(j).start()

        def tile(i, _):
            t = lax.rem(i + chip, chips)
            finish(t, s * rows, tuple((m_st[t, g], l_st[t, g], acc_st[t, g]) for g in range(heads)))

            @pl.when(s == 1)
            def _():
                for j in range(2):
                    d = n - 1 - (2 * t + j)

                    @pl.when(d == me)
                    def _():
                        own_result(1).start()

                    @pl.when(d != me)
                    def _():
                        result(1, d, me).start()

            return 0

        lax.fori_loop(0, chips, tile, 0)
        return 0

    lax.fori_loop(0, 2, half, 0)
    for j in range(len(saves)):
        save(j).wait()
    for s in gathers:
        for j, (target, p) in enumerate(own_sends):
            remote(s, me, p, target, own_sem.at[s, j]).wait_send()
        for way in range(2):
            forward(s, way).wait_send()
        for j in range(3):
            for p in range(2):
                relay(s, j, p).wait_send()
    for s in range(2):
        own_result(s).wait()
        for d in range(1, n):
            other = lax.rem(me + d, n)
            result(s, other, me).wait_send()
            result(s, other, other).wait_recv()


def front(x, gain, tables, w_query, w_key, w_value, n, layer):
    first = layer == 0
    rows, model = x.shape
    num_layers, _, all_heads, dim = w_query.shape
    more = layer < num_layers - 1
    heads = all_heads // n
    width = heads * dim
    block = rows // 2
    seq = n * rows
    vmem = pl.BlockSpec(memory_space=pltpu.VMEM)
    hbm = pl.BlockSpec(memory_space=pl.ANY)
    chips = n // 2
    out = jax.ShapeDtypeStruct((2, block, all_heads * dim), BF16)
    kv = jax.ShapeDtypeStruct((seq, width), BF16)
    table = jax.ShapeDtypeStruct((seq, dim), F32)
    packed = jax.ShapeDtypeStruct((model, 3 * width), BF16)
    dma = pltpu.SemaphoreType.DMA
    pos_scratch = [pltpu.VMEM((n,) + tables[0].shape, jnp.int32), dma((n,)), dma((n,))] if first else [dma((chips,))]
    by_head = [w.reshape(num_layers, model, n, heads, dim) for w in (w_query, w_key, w_value)]
    return pl.pallas_call(
        functools.partial(front_kernel, n, heads, dim, layer, first, more),
        name="front",
        out_shape=[out, kv, kv] + [table, table] * first + [packed] * more,
        in_specs=[vmem] * (4 if first else 2) + [hbm] * (3 if first else 7),
        out_specs=[hbm] * (3 + 2 * first + more),
        scratch_shapes=[pltpu.VMEM(packed.shape, BF16)] * more
        + pos_scratch
        + [
            pltpu.VMEM((2, n, block, model), BF16),
            pltpu.VMEM((3, model, heads, dim), BF16),
            pltpu.VMEM((model, 3 * width), BF16),
            pltpu.VMEM((seq, width), BF16),
            pltpu.VMEM((seq, width), BF16),
            pltpu.VMEM((seq, width), BF16),
            pltpu.VMEM((width, seq), BF16),
            pltpu.VMEM((seq, dim), F32),
            pltpu.VMEM((seq, dim), F32),
            pltpu.VMEM((seq, width), BF16),
            pltpu.VMEM((chips, heads, 1, TQ), F32),
            pltpu.VMEM((chips, heads, 1, TQ), F32),
            pltpu.VMEM((chips, heads, dim, TQ), F32),
            dma((3,)),
            dma((5,)),
            dma((3,)),
            dma((2, n, 2)),
            dma((2, 6)),
            dma((2, 2)),
            dma((2, 3, 2)),
            dma((2,)),
            dma((2, n)),
            dma((2, n)),
        ],
        compiler_params=pltpu.CompilerParams(vmem_limit_bytes=62 * MIB, collective_id=layer + 1, has_side_effects=True),
        cost_estimate=pl.CostEstimate(flops=6 * seq * model * width + 2 * seq * seq * width, bytes_accessed=seq * model * 2, transcendentals=seq * seq * heads // 2),
    )(x, gain, *tables, *by_head)


def mlp_parts(acc, normed, act, wg_ref, wu_ref, wd_ref, now):
    def gate_up(slot=0):
        h = normed[...]
        gate = jnp.dot(h, wg_ref[slot], preferred_element_type=F32)
        up = jnp.dot(h, wu_ref[slot], preferred_element_type=F32)
        act[now] = (jax.nn.silu(gate) * up).astype(BF16)

    def down(slot=0):
        acc[...] += jnp.dot(act[1 - now], wd_ref[slot], preferred_element_type=F32)

    return gate_up, down


def out_step(r, out_steps, layer, x_ref, o_ref, wo_ref, gain_ref, acc, normed):
    o = o_ref[...].reshape(acc.shape[0], o_ref.shape[2])
    part = jnp.dot(o, wo_ref[0], preferred_element_type=F32)

    @pl.when(r == 0)
    def _():
        acc[...] = part

    @pl.when(r > 0)
    def _():
        acc[...] += part

    @pl.when(r == out_steps - 1)
    def _():
        x = (x_ref[...].astype(F32) + acc[...]).astype(BF16)
        normed[...] = rms_norm(x, gain_ref[layer : layer + 1, :])
        acc[...] = x.astype(F32)


def last_kernel(
    out_steps, layer, x_ref, o_ref, wo_ref, gain_ref, wg_ref, wu_ref, wd_ref, *refs
):
    kv_refs = refs[: 2 * (layer + 1)]
    y_ref, kc_ref, vc_ref, acc, normed, act, mixed = refs[2 * (layer + 1) :]
    i = pl.program_id(0)
    last = pl.num_programs(0) - 1
    gate_up, down = mlp_parts(acc, normed, act, wg_ref, wu_ref, wd_ref, lax.rem(i, 2))

    @pl.when(i < out_steps)
    def _():
        out_step(i, out_steps, layer, x_ref, o_ref, wo_ref, gain_ref, acc, normed)

    def caches():
        dim = kc_ref.shape[2]
        for j, src in enumerate(kv_refs):
            count, heads = src.shape[0], src.shape[1] // dim
            for g in range(heads):
                mixed[j, pl.ds(g, count, stride=heads), :] = src[:, g * dim : (g + 1) * dim].astype(F32)
            (kc_ref, vc_ref)[j % 2][j // 2] = mixed[j].astype(BF16)

    @pl.when(i == out_steps)
    def _():
        gate_up()
        caches()

    @pl.when((i > out_steps) & (i < last))
    def _():
        down()
        gate_up()
        caches()

    @pl.when(i == last)
    def _():
        down()
        y_ref[...] = acc[...].astype(BF16)


def split_kernel(
    n, out_steps, layer, steps, x_ref, o_ref, wo_ref, gain_ref, next_gain_ref, wg_ref, wu_ref, wd_ref,
    y_ref, ha_ref, acc, normed, act, mine, wg_buf, wu_buf, wd_buf, w_sem, local_sem, recv_sem, own_sem, fwd_sem, relay_sem,
):
    i = pl.program_id(0)
    s, r = i // steps, lax.rem(i, steps)
    gate_up, down = mlp_parts(acc, normed, act, wg_buf, wu_buf, wd_buf, lax.rem(i, 2))
    slots, tf = wd_buf.shape[:2]
    slices = steps - out_steps - 1

    def load(kind, f):
        cols = pl.ds(pl.multiple_of(f * tf, tf), tf)
        src = (wg_ref.at[layer, :, cols], wu_ref.at[layer, :, cols], wd_ref.at[layer, cols])[kind]
        slot = lax.rem(f, slots)
        return pltpu.make_async_copy(src, (wg_buf, wu_buf, wd_buf)[kind].at[slot], w_sem.at[kind, slot])

    def slice_at(j):
        return jnp.where(s == 0, j, slices - 1 - j)

    def await_loads(kinds, f):
        @pl.when((s == 0) | (f < slices - slots))
        def _():
            for kind in kinds:
                load(kind, f).wait()

    def refill(kinds, f):
        after = jnp.where(s == 0, f + slots, f - slots)

        @pl.when((after >= 0) & (after < slices))
        def _():
            for kind in kinds:
                load(kind, after).start()

    f_up = slice_at(r - out_steps)
    f_down = slice_at(r - out_steps - 1)

    @pl.when(i == 0)
    def _():
        for f in range(slots):
            for kind in range(3):
                load(kind, f).start()
    piece = mine.shape[0] // 2
    chips = n // 2
    me = lax.axis_index("cp")
    chip, core = me // 2, lax.rem(me, 2)

    def at(step, k):
        return 2 * lax.rem(chip + step, chips) + k

    right, left, opp, partner = at(1, core), at(chips - 1, core), at(2, core), at(0, 1 - core)
    sources = (left, right, opp)
    own_sends = [(right, 0), (left, 1), (right, 1), (left, 0), (partner, 0), (partner, 1)]
    barrier = pltpu.get_barrier_semaphore()

    def remote(src, origin, p, target, sem):
        return pltpu.make_async_remote_copy(
            src_ref=src, dst_ref=ha_ref.at[origin, pl.ds(p * piece, piece)], send_sem=sem,
            recv_sem=recv_sem.at[origin, p], device_id={"cp": target}, device_id_type=MESH,
        )

    def held(origin, p):
        return ha_ref.at[origin, pl.ds(p * piece, piece)]

    def own(j):
        target, p = own_sends[j]
        return remote(mine.at[pl.ds(p * piece, piece)], me, p, target, own_sem.at[j])

    def keep():
        return pltpu.make_async_copy(mine, ha_ref.at[me], local_sem)

    def arrived(origin, p):
        remote(held(origin, p), origin, p, partner, own_sem.at[0]).wait_recv()

    def relay(j, p):
        return remote(held(sources[j], p), sources[j], p, partner, relay_sem.at[j, p])

    def forward(way):
        origin = (left, right)[way]
        return remote(held(origin, way), origin, way, (right, left)[way], fwd_sem.at[way])

    @pl.when(i == 0)
    def _():
        for d in range(1, n):
            pl.semaphore_signal(barrier, inc=1, device_id={"cp": lax.rem(me + d, n)}, device_id_type=MESH)
        pl.semaphore_wait(barrier, n - 1)

    @pl.when(i == steps + out_steps + 5)
    def _():
        for way in range(2):
            arrived((left, right)[way], way)
            forward(way).start()
            relay(way, way).start()

    @pl.when(i == steps + out_steps + 11)
    def _():
        for way in range(2):
            arrived((left, right)[way], 1 - way)
            relay(way, 1 - way).start()

    @pl.when(i == 2 * steps - 1)
    def _():
        for p in range(2):
            arrived(opp, p)
            relay(2, p).start()

    @pl.when(r < out_steps)
    def _():
        out_step(r, out_steps, layer, x_ref, o_ref, wo_ref, gain_ref, acc, normed)

    @pl.when((r >= out_steps) & (r < steps - 1))
    def _():
        await_loads((0, 1), f_up)

    @pl.when(r > out_steps)
    def _():
        await_loads((2,), f_down)

    @pl.when(r == out_steps)
    def _():
        gate_up(lax.rem(f_up, slots))

    @pl.when((r > out_steps) & (r < steps - 1))
    def _():
        down(lax.rem(f_down, slots))
        gate_up(lax.rem(f_up, slots))

    @pl.when(r == steps - 1)
    def _():
        down(lax.rem(f_down, slots))
        y_ref[...] = acc[...].astype(BF16)

    @pl.when((r >= out_steps) & (r < steps - 1))
    def _():
        refill((0, 1), f_up)

    @pl.when(r > out_steps)
    def _():
        refill((2,), f_down)

    @pl.when(i == steps - 1)
    def _():
        mine[...] = rms_norm(y_ref[...], next_gain_ref[layer + 1 : layer + 2, :])
        keep().start()
        for j in range(len(own_sends)):
            own(j).start()

    @pl.when(i == 2 * steps - 1)
    def _():
        keep().wait()
        for j in range(len(own_sends)):
            own(j).wait_send()
        for way in range(2):
            forward(way).wait_send()
        for j in range(3):
            for p in range(2):
                relay(j, p).wait_send()
        for origin in (partner, at(chips - 1, 1 - core), at(1, 1 - core), at(2, 1 - core)):
            for p in range(2):
                arrived(origin, p)


def tail_specs(layer, out_steps, slices, tf, model, step, r_of):
    out_at = lambda i: jnp.minimum(r_of(i), out_steps - 1)
    mlp_at = lambda i: jnp.clip(r_of(i) - out_steps, 0, slices - 1)
    down_at = lambda i: jnp.clip(r_of(i) - out_steps - 1, 0, slices - 1)
    w_out = pl.BlockSpec((1, step, model), lambda i: (layer, out_at(i), 0))
    mlp = [
        pl.BlockSpec((1, model, tf), lambda i: (layer, 0, mlp_at(i))),
        pl.BlockSpec((1, model, tf), lambda i: (layer, 0, mlp_at(i))),
        pl.BlockSpec((1, tf, model), lambda i: (layer, down_at(i), 0)),
    ]
    return out_at, mlp_at, w_out, mlp


def split_tail(x, o, n, w_out, gain, next_gain, w_gate, w_up, w_down, layer):
    rows, model = x.shape
    _, half, inner = o.shape
    ffn = w_gate.shape[2]
    out_steps, tf, slots = 2, TF, SLOTS
    slices = ffn // tf
    step = inner // out_steps
    steps = out_steps + slices + 1
    out_at, _, wo_spec, _ = tail_specs(layer, out_steps, slices, tf, model, step, lambda i: lax.rem(i, steps))
    hbm = pl.BlockSpec(memory_space=pl.ANY)
    part = pl.BlockSpec((half, model), lambda i: (i // steps, 0))
    full = pl.BlockSpec(gain.shape, lambda i: (0, 0))
    dma = pltpu.SemaphoreType.DMA
    return pl.pallas_call(
        functools.partial(split_kernel, n, out_steps, layer, steps),
        name="tail_split",
        grid=(2 * steps,),
        out_shape=[jax.ShapeDtypeStruct((rows, model), BF16), jax.ShapeDtypeStruct((n, half, model), BF16)],
        in_specs=[part, pl.BlockSpec((1, half, step), lambda i: (i // steps, 0, out_at(i))), wo_spec, full, full, hbm, hbm, hbm],
        out_specs=[part, pl.BlockSpec(memory_space=pl.ANY)],
        scratch_shapes=[
            pltpu.VMEM((half, model), F32),
            pltpu.VMEM((half, model), BF16),
            pltpu.VMEM((2, half, tf), BF16),
            pltpu.VMEM((half, model), BF16),
            pltpu.VMEM((slots, model, tf), BF16),
            pltpu.VMEM((slots, model, tf), BF16),
            pltpu.VMEM((slots, tf, model), BF16),
            dma((3, slots)),
            dma,
            dma((n, 2)),
            dma((6,)),
            dma((2,)),
            dma((3, 2)),
        ],
        compiler_params=pltpu.CompilerParams(vmem_limit_bytes=63 * MIB, collective_id=8 + layer, has_side_effects=True),
        cost_estimate=pl.CostEstimate(
            flops=2 * rows * model * (inner + 3 * ffn), bytes_accessed=4 * model * (inner + 3 * ffn), transcendentals=rows * ffn
        ),
    )(x, o, w_out.reshape(w_out.shape[0], inner, model), gain, next_gain, w_gate, w_up, w_down)


def last_tail(x, o, kvs, heads, w_out, gain, w_gate, w_up, w_down, layer):
    rows, model = x.shape
    _, half, inner = o.shape
    ffn = w_gate.shape[2]
    out_steps, tf = 4, TF
    slices = ffn // tf
    step = inner // out_steps
    seq, width = kvs[0].shape
    dim = width // heads
    part = seq // slices
    out_at, mlp_at, wo_spec, mlp_specs = tail_specs(layer, out_steps, slices, tf, model, step, lambda i: i)
    whole = pl.BlockSpec((rows, model), lambda i: (0, 0))
    cache = jax.ShapeDtypeStruct((layer + 1, seq * heads, dim), BF16)
    cache_spec = pl.BlockSpec((layer + 1, part * heads, dim), lambda i: (0, mlp_at(i), 0))
    return pl.pallas_call(
        functools.partial(last_kernel, out_steps, layer),
        name="tail_last",
        grid=(out_steps + slices + 1,),
        out_shape=[jax.ShapeDtypeStruct((rows, model), BF16), cache, cache],
        in_specs=[
            whole,
            pl.BlockSpec((2, half, step), lambda i: (0, 0, out_at(i))),
            wo_spec,
            pl.BlockSpec(gain.shape, lambda i: (0, 0)),
        ]
        + mlp_specs
        + [pl.BlockSpec((part, width), lambda i: (mlp_at(i), 0))] * len(kvs),
        out_specs=[whole, cache_spec, cache_spec],
        scratch_shapes=[
            pltpu.VMEM((rows, model), F32),
            pltpu.VMEM((rows, model), BF16),
            pltpu.VMEM((2, rows, tf), BF16),
            pltpu.VMEM((len(kvs), part * heads, dim), F32),
        ],
        compiler_params=pltpu.CompilerParams(vmem_limit_bytes=60 * MIB),
        cost_estimate=pl.CostEstimate(
            flops=2 * rows * model * (inner + 3 * ffn), bytes_accessed=2 * model * (inner + 3 * ffn), transcendentals=rows * ffn
        ),
    )(x, o, w_out.reshape(w_out.shape[0], inner, model), gain, w_gate, w_up, w_down, *kvs)


def solution(mesh):
    cp_size = mesh.shape["cp"]
    row_spec = P(("req", "cp"), None)
    pos_spec = P(("req", "cp"))
    rep_spec = P()
    cache_spec = P(None, "req", "cp", None)

    def per_device(hidden, positions, gain_attn, gain_mlp, w_query, w_key, w_value, w_out, w_gate, w_up, w_down):
        num_layers, model, all_heads, dim = w_query.shape
        rows = hidden.shape[0]
        cache_shape = (num_layers, cp_size * rows, all_heads // cp_size, dim)
        inv_freq = ROPE_BASE ** (-jnp.arange(0, dim, 2, dtype=F32) / dim)
        tables = [positions.reshape(rows // 128, 128), jnp.concatenate([inv_freq, inv_freq])[None]]
        kvs = []
        for layer in range(num_layers):
            o, k, v, *new = front(hidden, gain_attn, tables, w_query, w_key, w_value, cp_size, layer)
            kvs += [k, v]
            if layer == 0:
                cos_sin, new = new[:2], new[2:]
            if layer < num_layers - 1:
                hidden, gathered = split_tail(hidden, o, cp_size, w_out, gain_mlp, gain_attn, w_gate, w_up, w_down, layer)
                tables = cos_sin + new + [gathered]
            else:
                hidden, k_cache, v_cache = last_tail(
                    hidden, o, kvs, all_heads // cp_size, w_out, gain_mlp, w_gate, w_up, w_down, layer
                )
        return hidden, k_cache.reshape(cache_shape), v_cache.reshape(cache_shape)

    in_specs = (row_spec, pos_spec) + (rep_spec,) * 9
    return jax.shard_map(per_device, mesh=mesh, in_specs=in_specs, out_specs=(row_spec, cache_spec, cache_spec), check_vma=False)
```
